8 devices in a mesh: dp: 2 (over z, y), tp: 4 (over x, core).
Axes of the slice: x: 2, y: 2, z: 1, core: 2. Of those that a mesh axis runs over, the one named last changes fastest.
Arguments:
- hidden: bfloat16 [2, 256, 2048], P('dp'), parts along dimension 0
- norm_w: bfloat16 [2, 2048], replicated
- w_z: bfloat16 [2, 2048, 4096], P(None, None, 'tp')
- w_x: bfloat16 [2, 2048, 4096], P(None, None, 'tp')
- w_bc: bfloat16 [2, 2048, 128], replicated
- w_dt: bfloat16 [2, 2048, 64], P(None, None, 'tp')
- conv_x: bfloat16 [2, 4, 4096], P(None, None, 'tp')
- conv_bc: bfloat16 [2, 4, 128], replicated
- bias_x: bfloat16 [2, 4096], P(None, 'tp')
- bias_bc: bfloat16 [2, 128], replicated
- dt_bias: float32 [2, 64], P(None, 'tp')
- a_log: float32 [2, 64], P(None, 'tp')
- d_skip: float32 [2, 64], P(None, 'tp')
- gate_w: bfloat16 [2, 4096], P(None, 'tp')
- w_out: bfloat16 [2, 4096, 2048], P(None, 'tp')
Outputs:
- output: bfloat16 [2, 256, 2048], P('dp'), parts along dimension 0
There are 2 independent parts. The reference program is written for one: setup_inputs(seed, part) draws one part's arguments, and reference() takes and returns one part's arrays. A program takes and returns all parts, laid end to end along the dimension named above; an argument that names none is the same for every part.
All inputs are finite; a program needn't handle non-finite values.
Results may differ from the reference program's by a relative error of at most 0.0143168.
Values sent between devices are 32-bit elements.
A program may use at most 1 GiB of HBM per device.

```python
import math
import jax
import jax.numpy as jnp
from jax import lax

BATCH_ROWS = 1
SEQ_LEN = 256
D_MODEL = 2048
HEADS = 64
HEAD_DIM = 64
STATE_DIM = 64
LAYERS = 2
CONV_WIDTH = 4
BLOCK_LEN = 256

INNER_WIDTH = HEADS * HEAD_DIM
EPSILON = 1e-5


def setup_inputs(seed: int = 0, part: int = 0) -> dict:
    key_list = jax.random.split(jax.random.key(seed), 16)
    part_key = jax.random.fold_in(jax.random.key(seed + 1), part)
    in_scale = D_MODEL ** -0.5
    hidden = jax.random.normal(part_key, (BATCH_ROWS, SEQ_LEN, D_MODEL), jnp.float32)
    head_scale = jnp.exp(jax.random.uniform(key_list[0], (LAYERS, HEADS), jnp.float32, -1.2, 1.2))
    col_scale = jnp.repeat(head_scale, HEAD_DIM, axis=1)[:, None, :]
    dt_init = jnp.exp(jax.random.uniform(key_list[1], (LAYERS, HEADS), jnp.float32, math.log(0.001), math.log(0.1)))
    return {
        'hidden': hidden.astype(jnp.bfloat16),
        'norm_w': (1.0 + 0.2 * jax.random.normal(key_list[2], (LAYERS, D_MODEL), jnp.float32)).astype(jnp.bfloat16),
        'w_z': (in_scale * jax.random.normal(key_list[3], (LAYERS, D_MODEL, INNER_WIDTH), jnp.float32)).astype(jnp.bfloat16),
        'w_x': (in_scale * col_scale * jax.random.normal(key_list[4], (LAYERS, D_MODEL, INNER_WIDTH), jnp.float32)).astype(jnp.bfloat16),
        'w_bc': (in_scale * jax.random.normal(key_list[5], (LAYERS, D_MODEL, 2 * STATE_DIM), jnp.float32)).astype(jnp.bfloat16),
        'w_dt': (0.5 * in_scale * jax.random.normal(key_list[6], (LAYERS, D_MODEL, HEADS), jnp.float32)).astype(jnp.bfloat16),
        'conv_x': (0.5 * jax.random.normal(key_list[7], (LAYERS, CONV_WIDTH, INNER_WIDTH), jnp.float32)).astype(jnp.bfloat16),
        'conv_bc': (0.5 * jax.random.normal(key_list[8], (LAYERS, CONV_WIDTH, 2 * STATE_DIM), jnp.float32)).astype(jnp.bfloat16),
        'bias_x': (0.3 * jax.random.normal(key_list[9], (LAYERS, INNER_WIDTH), jnp.float32)).astype(jnp.bfloat16),
        'bias_bc': (0.3 * jax.random.normal(key_list[10], (LAYERS, 2 * STATE_DIM), jnp.float32)).astype(jnp.bfloat16),
        'dt_bias': dt_init + jnp.log(-jnp.expm1(-dt_init)),
        'a_log': jnp.log(jax.random.uniform(key_list[11], (LAYERS, HEADS), jnp.float32, 1.0, 16.0)),
        'd_skip': jax.random.uniform(key_list[12], (LAYERS, HEADS), jnp.float32, 0.5, 2.0),
        'gate_w': (1.0 + 0.2 * jax.random.normal(key_list[13], (LAYERS, INNER_WIDTH), jnp.float32)).astype(jnp.bfloat16),
        'w_out': (INNER_WIDTH ** -0.5 * jax.random.normal(key_list[14], (LAYERS, INNER_WIDTH, D_MODEL), jnp.float32)).astype(jnp.bfloat16),
    }


def causal_conv(seq_in, kernel, conv_bias):
    n_steps = seq_in.shape[1]
    padded = jnp.pad(seq_in, ((0, 0), (CONV_WIDTH - 1, 0), (0, 0)))
    conv_sum = conv_bias.astype(jnp.float32)
    for tap_index in range(CONV_WIDTH):
        conv_sum = conv_sum + padded[:, tap_index:tap_index + n_steps, :].astype(jnp.float32) * kernel[tap_index].astype(jnp.float32)
    return conv_sum


def ssd_sequence(seq_in):
    x_heads, dt_val, a_vals, b_in, c_in = seq_in
    n_blocks = SEQ_LEN // BLOCK_LEN
    step_ids = jnp.arange(BLOCK_LEN)
    lower_tri = step_ids[:, None] >= step_ids[None, :]

    def block_step(state, block):
        x_block, dt_block, a_block, b_block, c_block = block
        a_cum = jnp.cumsum(a_block, axis=0)
        seg_sum = a_cum[:, None, :] - a_cum[None, :, :]
        decay_mat = jnp.where(lower_tri[:, :, None], jnp.exp(jnp.minimum(seg_sum, 0.0)), 0.0)
        c_dot_b = jnp.einsum('in,jn->ij', c_block, b_block)
        x_dt = x_block * dt_block[:, :, None]
        y_in = jnp.einsum('ijh,jhp->ihp', decay_mat * c_dot_b[:, :, None], x_dt)
        y_st = jnp.einsum('in,hpn->ihp', c_block, state) * jnp.exp(a_cum)[:, :, None]
        tail_decay = jnp.exp(a_cum[-1][None, :] - a_cum)
        new_state = state * jnp.exp(a_cum[-1])[:, None, None] + jnp.einsum('jn,jhp->hpn', b_block, x_dt * tail_decay[:, :, None])
        return new_state, y_in + y_st

    blocks_in = (
        x_heads.reshape(n_blocks, BLOCK_LEN, HEADS, HEAD_DIM),
        dt_val.reshape(n_blocks, BLOCK_LEN, HEADS),
        a_vals.reshape(n_blocks, BLOCK_LEN, HEADS),
        b_in.reshape(n_blocks, BLOCK_LEN, STATE_DIM),
        c_in.reshape(n_blocks, BLOCK_LEN, STATE_DIM),
    )
    init_state = jnp.zeros((HEADS, HEAD_DIM, STATE_DIM), jnp.float32)
    last_state, y_blocks = lax.scan(block_step, init_state, blocks_in)
    return y_blocks.reshape(SEQ_LEN, HEADS, HEAD_DIM)


def mixer_layer(current, layer_params):
    norm_w, w_z, w_x, w_bc, w_dt, conv_x, conv_bc, bias_x, bias_bc, dt_bias, a_log, d_skip, gate_w, w_out = layer_params
    tokens = BATCH_ROWS * SEQ_LEN
    residual = current.astype(jnp.float32)
    normed = (residual * lax.rsqrt(jnp.mean(residual * residual, axis=-1, keepdims=True) + EPSILON) * norm_w.astype(jnp.float32)).astype(jnp.bfloat16)
    flat_in = normed.reshape(tokens, D_MODEL)
    gate_z = jnp.dot(flat_in, w_z, preferred_element_type=jnp.float32).astype(jnp.bfloat16)
    x_pre = jnp.dot(flat_in, w_x, preferred_element_type=jnp.float32).astype(jnp.bfloat16)
    bc_pre = jnp.dot(flat_in, w_bc, preferred_element_type=jnp.float32).astype(jnp.bfloat16)
    dt_pre = jnp.dot(flat_in, w_dt, preferred_element_type=jnp.float32).astype(jnp.bfloat16)
    x_act = jax.nn.silu(causal_conv(x_pre.reshape(BATCH_ROWS, SEQ_LEN, INNER_WIDTH), conv_x, bias_x))
    bc_act = jax.nn.silu(causal_conv(bc_pre.reshape(BATCH_ROWS, SEQ_LEN, 2 * STATE_DIM), conv_bc, bias_bc))
    dt_val = jax.nn.softplus(dt_pre.astype(jnp.float32).reshape(BATCH_ROWS, SEQ_LEN, HEADS) + dt_bias)
    a_vals = -dt_val * jnp.exp(a_log)
    x_heads = x_act.reshape(BATCH_ROWS, SEQ_LEN, HEADS, HEAD_DIM)
    y_heads = lax.map(ssd_sequence, (x_heads, dt_val, a_vals, bc_act[..., :STATE_DIM], bc_act[..., STATE_DIM:]))
    y_heads = y_heads + d_skip[:, None] * x_heads
    gated_v = y_heads.reshape(BATCH_ROWS, SEQ_LEN, INNER_WIDTH) * jax.nn.silu(gate_z.astype(jnp.float32).reshape(BATCH_ROWS, SEQ_LEN, INNER_WIDTH))
    normed_y = (gated_v * lax.rsqrt(jnp.mean(gated_v * gated_v, axis=-1, keepdims=True) + EPSILON) * gate_w.astype(jnp.float32)).astype(jnp.bfloat16)
    mixed_out = jnp.dot(normed_y.reshape(tokens, INNER_WIDTH), w_out, preferred_element_type=jnp.float32)
    return (residual + mixed_out.reshape(BATCH_ROWS, SEQ_LEN, D_MODEL)).astype(jnp.bfloat16)


def reference(hidden, norm_w, w_z, w_x, w_bc, w_dt, conv_x, conv_bc, bias_x, bias_bc, dt_bias, a_log, d_skip, gate_w, w_out):
    params = (norm_w, w_z, w_x, w_bc, w_dt, conv_x, conv_bc, bias_x, bias_bc, dt_bias, a_log, d_skip, gate_w, w_out)

    def layer_step(current, layer_params):
        return mixer_layer(current, layer_params), None

    final_hidden, unused = lax.scan(layer_step, hidden, params)
    return final_hidden
```

```python
import functools

import jax
import jax.numpy as jnp
from jax import lax
from jax.experimental import pallas as pl
from jax.experimental.pallas import tpu as pltpu
from jax.sharding import PartitionSpec as P

EPSILON = 1e-5
MESH = pl.DeviceIdType.MESH
CHUNK = 64
PIECE = 256
EXTRA = 8
HEAD = 64
F32 = jnp.float32
BF16 = jnp.bfloat16


def split3(val):
    hi = val.astype(BF16).astype(F32)
    rest = val - hi
    mid = rest.astype(BF16).astype(F32)
    return hi, mid, rest - mid


def stack3(val):
    return jnp.concatenate(split3(val), axis=0).astype(BF16)


def dot(a, b):
    return lax.dot_general(a, b, (((1,), (0,)), ((), ())), preferred_element_type=F32)


def dot_nt(a, b):
    return lax.dot_general(a, b, (((1,), (1,)), ((), ())), preferred_element_type=F32)


def exact_dot(a_stack, b_parts, product=dot):
    rows = a_stack.shape[0] // 3
    b_hi, b_mid, b_lo = b_parts
    r1 = product(a_stack, b_hi)
    r2 = product(a_stack[: 2 * rows], b_mid)
    r3 = product(a_stack[:rows], b_lo)
    small = r1[2 * rows :] + r2[rows:] + r3
    return r1[:rows] + (r1[rows : 2 * rows] + r2[:rows] + small)


def iota(shape, dim):
    return lax.broadcasted_iota(jnp.int32, shape, dim)


def kernel(inner, hid_h, nw_h, wz_h, wx_h, wbc_h, wdt_h, cx_h, cbc_h, bx_h, bbc_h, dtb_h, al_h, ds_h, gw_h, wo_h,
           out_ref, hid, nw, wz, wx, wbc, wdt, cx, cbc, bx, bbc, dtb, al, ds, gw, wo,
           ubuf, psend, prcv, qbuf, own, hbuf, x0s, q0s, xs, vs, state, gbuf,
           small_sem, hid_sem, w_sem, ps_sem, pr_sem, qs_sem, qr_sem, us_sem, ur_sem):
    me = lax.axis_index("tp")
    core = me % 2
    chip = me // 2
    peer = me + 1 - 2 * core
    cross = (me + 2) % 4
    n_chunks = hid_h.shape[1] // CHUNK
    n_piece = wx_h.shape[2] // PIECE
    layers = nw_h.shape[0]
    local = wx_h.shape[2]
    half = wo_h.shape[2] // 2

    barrier = pltpu.get_barrier_semaphore()
    for other in (peer, cross):
        pl.semaphore_signal(barrier, inc=1, device_id={"tp": other}, device_id_type=MESH)

    smalls = [pltpu.make_async_copy(src, dst, small_sem.at[i]) for i, (src, dst) in enumerate(
        [(nw_h, nw), (cx_h, cx), (cbc_h, cbc), (bx_h, bx), (bbc_h, bbc), (dtb_h, dtb), (al_h, al), (ds_h, ds), (gw_h, gw), (wdt_h, wdt)])]

    def hid_copy(c):
        return pltpu.make_async_copy(hid_h.at[0, pl.ds(c * CHUNK, CHUNK)], hid.at[c], hid_sem.at[c])

    def weight_copies(layer):
        cols = lambda n: pl.ds(n * PIECE, PIECE)
        bc = pltpu.make_async_copy(wbc_h.at[layer], wbc.at[layer], w_sem.at[layer, 0])
        xcp = [pltpu.make_async_copy(wx_h.at[layer, :, cols(n)], wx.at[layer, n], w_sem.at[layer, 1 + n]) for n in range(n_piece)]
        zcp = [pltpu.make_async_copy(wz_h.at[layer, :, cols(n)], wz.at[layer, n], w_sem.at[layer, 5 + n]) for n in range(n_piece)]
        ocp = []
        for side in range(2):
            for n in range(n_piece):
                ocp.append(pltpu.make_async_copy(wo_h.at[layer, :, cols(side * n_piece + n)], wo.at[layer, side, n], w_sem.at[layer, 9 + side * n_piece + n]))
        return bc, xcp, zcp, ocp

    hid_copy(0).start()
    for cp in smalls:
        cp.start()
    first_w = weight_copies(0)
    first_w[0].start()
    for group in first_w[1:]:
        for cp in group:
            cp.start()
    for c in range(1, n_chunks):
        hid_copy(c).start()

    def rows_of(m):
        return CHUNK + EXTRA if m == 0 else CHUNK

    def p_copy(s, m):
        part = pl.ds(0, rows_of(m))
        return pltpu.make_async_remote_copy(src_ref=psend.at[s, m, part], dst_ref=prcv.at[s, m, part], send_sem=ps_sem.at[s, m],
                                            recv_sem=pr_sem.at[s, m], device_id={"tp": peer}, device_id_type=MESH)

    def q_copy(s, m):
        part = pl.ds(0, rows_of(m))
        return pltpu.make_async_remote_copy(src_ref=qbuf.at[chip, s, m, part], dst_ref=qbuf.at[chip, s, m, part], send_sem=qs_sem.at[s, m],
                                            recv_sem=qr_sem.at[s, m], device_id={"tp": cross}, device_id_type=MESH)

    def u_copy(layer, c, m):
        s = layer * n_chunks + c
        return pltpu.make_async_remote_copy(src_ref=ubuf.at[layer + 1, core, c, m], dst_ref=ubuf.at[layer + 1, core, c, m], send_sem=us_sem.at[s, m],
                                            recv_sem=ur_sem.at[s, m], device_id={"tp": peer}, device_id_type=MESH)

    row64 = iota((CHUNK, PIECE), 0)
    lane64 = iota((CHUNK, PIECE), 1) % HEAD
    eye = row64 == lane64
    causal = row64 >= lane64
    low_head = iota((CHUNK, 128), 1) < HEAD

    def to_row(col):
        return jnp.sum(jnp.where(eye, col, 0.0), axis=0, keepdims=True)

    def to_col(row):
        return jnp.sum(jnp.where(eye[:, :HEAD], row[:, :HEAD], 0.0), axis=1, keepdims=True)

    def scale_of(square_sum):
        return lax.rsqrt(square_sum / inner + EPSILON) * (1.0 / 64.0)

    def inverse_of(square_sum):
        return jnp.where(square_sum < jnp.inf, 64.0 * jnp.sqrt(square_sum / inner + EPSILON), 0.0)

    def head_blocks(part):
        left, right = part[:, :128], part[:, 128:]
        none = jnp.zeros_like(left)
        rows = [jnp.concatenate([jnp.where(low_head, left, 0.0), none], axis=1), jnp.concatenate([jnp.where(low_head, 0.0, left), none], axis=1),
                jnp.concatenate([none, jnp.where(low_head, right, 0.0)], axis=1), jnp.concatenate([none, jnp.where(low_head, 0.0, right)], axis=1)]
        return jnp.concatenate(rows, axis=0).astype(BF16)

    def start_layer():
        state[...] = jnp.zeros_like(state)
        x0s[0:8] = jnp.zeros((8, local), F32)
        q0s[0:8] = jnp.zeros((8, q0s.shape[1]), F32)

    def tap_sum(buf, lanes, kern, bias):
        total = bias
        for j in range(4):
            total = total + buf[5 + j : 5 + j + CHUNK, lanes] * kern[j : j + 1].astype(F32)
        return total

    def step(layer, c, waits=None):
        s = layer * n_chunks + c
        bc_wait, x_wait, z_wait, o_wait = waits if waits is not None else (None, None, None, None)
        square = jnp.zeros((CHUNK, 1), F32)
        for side in range(2):
            for m in range(n_piece):
                val = ubuf[layer, side, c, m]
                square = square + jnp.sum(val * val, axis=1, keepdims=True)
        scale = lax.rsqrt(square / (2 * half) + EPSILON)
        norm_row = nw[layer : layer + 1].astype(F32)
        for side in range(2):
            for m in range(n_piece):
                at = side * half + m * PIECE
                hbuf[:, at : at + PIECE] = (ubuf[layer, side, c, m] * scale * norm_row[:, at : at + PIECE]).astype(BF16)
        if waits is not None:
            bc_wait.wait()
        q0s[8:, :] = dot(hbuf[...], wbc[layer]).astype(BF16).astype(F32)
        bc = jax.nn.silu(tap_sum(q0s, slice(None), cbc[layer], bbc[layer : layer + 1].astype(F32)))
        q0s[0:8] = q0s[CHUNK : CHUNK + 8]
        wdt3 = jnp.concatenate([wdt[layer]] * 3, axis=0)
        r_pre = dot_nt(hbuf[...], wdt3).astype(BF16).astype(F32)
        triple = lambda ref: jnp.concatenate([ref[layer : layer + 1]] * 3, axis=1)
        dt_in = r_pre + triple(dtb)
        dt_val = jnp.maximum(dt_in, 0.0) + jnp.log1p(jnp.exp(-jnp.abs(dt_in)))
        a_vals = -dt_val * jnp.exp(triple(al))
        tri = (iota((CHUNK, 3 * CHUNK), 0) >= iota((CHUNK, 3 * CHUNK), 1) % CHUNK).astype(F32).astype(BF16)
        a_cum = dot(tri, stack3(a_vals))
        skip = jnp.broadcast_to(triple(ds), (8, a_cum.shape[1]))
        to_spread = jnp.concatenate([dt_val, a_cum, skip], axis=0)
        hi, mid, lo = split3(to_spread)
        lane = iota(to_spread.shape, 1)
        n_heads = local // HEAD
        spread_in = jnp.where(lane < n_heads, hi, jnp.where(lane < 2 * n_heads, mid, lo)).astype(BF16)

        swapped = pltpu.roll(bc, HEAD, 1)
        c_stack = stack3(swapped[:, :HEAD])
        b_parts = split3(bc[:, :HEAD])
        cb = exact_dot(c_stack, [jnp.concatenate([part] * 4, axis=0).astype(BF16) for part in b_parts], dot_nt)
        bt_stack = stack3(jnp.transpose(bc)[:HEAD])

        gate_sq = jnp.zeros((CHUNK, 1), F32)
        for n in range(n_piece):
            at = slice(n * PIECE, (n + 1) * PIECE)
            if waits is not None:
                x_wait[n].wait()
            x0s[8:, at] = dot(hbuf[...], wx[layer, n]).astype(BF16).astype(F32)
            x_act = jax.nn.silu(tap_sum(x0s, at, cx[layer, :, at], bx[layer : layer + 1, at].astype(F32)))
            x0s[0:8, at] = x0s[CHUNK : CHUNK + 8, at]
            group = n * (PIECE // HEAD)
            pick = (iota((3 * n_heads, PIECE), 1) // HEAD + group == iota((3 * n_heads, PIECE), 0) % n_heads).astype(F32).astype(BF16)
            spread = dot(spread_in, pick)
            dt_e, a_e, skip_e = spread[:CHUNK], spread[CHUNK : 2 * CHUNK], spread[2 * CHUNK : 2 * CHUNK + 1]
            a_row = to_row(a_e)
            a_last = a_e[CHUNK - 1 : CHUNK]
            decay = jnp.where(causal, jnp.exp(jnp.minimum(a_e - a_row, 0.0)), 0.0) * cb
            x_dt = x_act * dt_e
            y = exact_dot(stack3(decay), [head_blocks(part) for part in split3(x_dt)])
            old = state[:, at]
            carried = exact_dot(c_stack, [part.astype(BF16) for part in split3(old)])
            y = y + carried * jnp.exp(a_e) + skip_e * x_act
            tail = x_dt * jnp.exp(a_last - a_e)
            state[:, at] = jnp.exp(a_last) * old + exact_dot(bt_stack, [part.astype(BF16) for part in split3(tail)])
            xs[:, at] = y
        for n in range(n_piece):
            at = slice(n * PIECE, (n + 1) * PIECE)
            if waits is not None:
                z_wait[n].wait()
            z = dot(hbuf[...], wz[layer, n]).astype(BF16).astype(F32)
            v = xs[:, at] * jax.nn.silu(z)
            vs[:, at] = v
            gate_sq = gate_sq + jnp.sum(v * v, axis=1, keepdims=True)
        scale = scale_of(gate_sq)
        gbuf[...] = (vs[...] * scale * gw[layer : layer + 1].astype(F32)).astype(BF16)
        psend[s, 0, CHUNK:] = jnp.broadcast_to(to_row(gate_sq), (EXTRA, PIECE))
        if waits is not None:
            for cp in o_wait:
                cp.wait()
            pl.semaphore_wait(barrier, 2)
        for m in range(n_piece):
            psend[s, m, 0:CHUNK] = dot(gbuf[...], wo[layer, 1 - core, m])
            p_copy(s, m).start()
        for m in range(n_piece):
            own[m] = dot(gbuf[...], wo[layer, core, m])
        for m in range(n_piece):
            p_copy(s, m).wait_recv()
            if m == 0:
                peer_sq = to_col(prcv[s, 0, CHUNK : CHUNK + 1])
                chip_sq = gate_sq + peer_sq
                chip_scale = scale_of(chip_sq)
                f_own = chip_scale * inverse_of(gate_sq)
                f_peer = chip_scale * inverse_of(peer_sq)
                qbuf[chip, s, 0, CHUNK:] = jnp.broadcast_to(to_row(chip_sq), (EXTRA, PIECE))
            qbuf[chip, s, m, 0:CHUNK] = own[m] * f_own + prcv[s, m, 0:CHUNK] * f_peer
            q_copy(s, m).start()

    def finish(layer, c, last):
        s = layer * n_chunks + c
        for m in range(n_piece):
            q_copy(s, m).wait_recv()
            if m == 0:
                sq0 = to_col(qbuf[0, s, 0, CHUNK : CHUNK + 1])
                sq1 = to_col(qbuf[1, s, 0, CHUNK : CHUNK + 1])
                norm = lax.rsqrt((sq0 + sq1) / inner + EPSILON)
                f0 = norm * inverse_of(sq0)
                f1 = norm * inverse_of(sq1)
            total = ubuf[layer, core, c, m] + (qbuf[0, s, m, 0:CHUNK] * f0 + qbuf[1, s, m, 0:CHUNK] * f1)
            new = total.astype(BF16)
            ubuf[layer + 1, core, c, m] = new.astype(F32)
            u_copy(layer, c, m).start()
            if last:
                out_ref[0, pl.ds(c * CHUNK, CHUNK), pl.ds(pl.multiple_of(core * half + m * PIECE, PIECE), PIECE)] = new
        for m in range(n_piece):
            u_copy(layer, c, m).wait_recv()
            if last:
                out_ref[0, pl.ds(c * CHUNK, CHUNK), pl.ds(pl.multiple_of((1 - core) * half + m * PIECE, PIECE), PIECE)] = ubuf[layer + 1, 1 - core, c, m].astype(BF16)

    def load_hidden(c):
        hid_copy(c).wait()
        for side in range(2):
            for m in range(n_piece):
                at = side * half + m * PIECE
                ubuf[0, side, c, m] = hid[c, :, at : at + PIECE].astype(F32)

    start_layer()
    load_hidden(0)
    for cp in smalls:
        cp.wait()
    step(0, 0, first_w)
    later = [weight_copies(layer) for layer in range(1, layers)]
    for groups in later:
        groups[0].start()
        for group in groups[1:]:
            for cp in group:
                cp.start()

    @pl.loop(1, n_chunks)
    def _(c):
        load_hidden(c)
        step(0, c)

    for layer in range(1, layers):
        start_layer()
        groups = later[layer - 1]
        groups[0].wait()
        for group in groups[1:]:
            for cp in group:
                cp.wait()

        @pl.loop(0, n_chunks)
        def _(c):
            finish(layer - 1, c, False)
            step(layer, c)

    @pl.loop(0, n_chunks)
    def _(c):
        finish(layers - 1, c, True)

    @pl.loop(0, layers * n_chunks)
    def _(s):
        for m in range(n_piece):
            p_copy(s, m).wait_send()
            q_copy(s, m).wait_send()
            u_copy(s // n_chunks, s % n_chunks, m).wait_send()


def solution(mesh):
    in_specs = (P('dp'), P(), P(None, None, 'tp'), P(None, None, 'tp'), P(), P(None, None, 'tp'), P(None, None, 'tp'), P(), P(None, 'tp'), P(),
                P(None, 'tp'), P(None, 'tp'), P(None, 'tp'), P(None, 'tp'), P(None, 'tp', None))
    tp_size = mesh.shape['tp']

    def device_forward(hidden, norm_w, w_z, w_x, w_bc, w_dt, conv_x, conv_bc, bias_x, bias_bc, dt_bias, a_log, d_skip, gate_w, w_out):
        layers, width, local = w_x.shape
        n_chunks = hidden.shape[1] // CHUNK
        n_piece = local // PIECE
        steps = layers * n_chunks
        bc_width = w_bc.shape[-1]
        w_dt = jnp.swapaxes(w_dt, 1, 2)
        vm = lambda shape, dtype: pltpu.VMEM(shape, dtype)
        same = lambda arr: pltpu.VMEM(arr.shape, arr.dtype)
        scratch = [
            vm((n_chunks, CHUNK, width), BF16), same(norm_w), vm((layers, n_piece, width, PIECE), BF16), vm((layers, n_piece, width, PIECE), BF16),
            same(w_bc), same(w_dt), same(conv_x), same(conv_bc), same(bias_x), same(bias_bc), same(dt_bias), same(a_log), same(d_skip), same(gate_w),
            vm((layers, 2, n_piece, local, PIECE), BF16),
            vm((layers + 1, 2, n_chunks, n_piece, CHUNK, PIECE), F32),
            vm((steps, n_piece, CHUNK + EXTRA, PIECE), F32), vm((steps, n_piece, CHUNK + EXTRA, PIECE), F32),
            vm((2, steps, n_piece, CHUNK + EXTRA, PIECE), F32),
            vm((n_piece, CHUNK, PIECE), F32), vm((CHUNK, width), BF16), vm((CHUNK + 8, local), F32), vm((CHUNK + 8, bc_width), F32),
            vm((CHUNK, local), F32), vm((CHUNK, local), F32), vm((HEAD, local), F32), vm((CHUNK, local), BF16),
            pltpu.SemaphoreType.DMA((10,)), pltpu.SemaphoreType.DMA((n_chunks,)), pltpu.SemaphoreType.DMA((layers, 9 + 2 * n_piece)),
        ] + [pltpu.SemaphoreType.DMA((steps, n_piece)) for _ in range(6)]
        return pl.pallas_call(
            functools.partial(kernel, float(local * tp_size)),
            out_shape=jax.ShapeDtypeStruct(hidden.shape, hidden.dtype),
            in_specs=[pl.BlockSpec(memory_space=pl.ANY)] * 15,
            out_specs=pl.BlockSpec(memory_space=pltpu.VMEM),
            scratch_shapes=scratch,
            compiler_params=pltpu.CompilerParams(collective_id=0, has_side_effects=True, vmem_limit_bytes=60 * 1024 * 1024),
        )(hidden, norm_w, w_z, w_x, w_bc, w_dt, conv_x, conv_bc, bias_x, bias_bc, dt_bias, a_log, d_skip, gate_w, w_out)

    return jax.shard_map(device_forward, mesh=mesh, in_specs=in_specs, out_specs=P('dp'), check_vma=False)
```

```python
import functools

import jax
import jax.numpy as jnp
from jax import lax
from jax.experimental import pallas as pl
from jax.experimental.pallas import tpu as pltpu
from jax.sharding import PartitionSpec as P

EPSILON = 1e-5
MESH = pl.DeviceIdType.MESH
CHUNK = 128
SUB = 64
PIECE = 256
EXTRA = 8
HEAD = 64
F32 = jnp.float32
BF16 = jnp.bfloat16


def split3(val):
    hi = val.astype(BF16).astype(F32)
    rest = val - hi
    mid = rest.astype(BF16).astype(F32)
    return hi, mid, rest - mid


def stack3(val):
    return jnp.concatenate(split3(val), axis=0).astype(BF16)


def dot(a, b):
    return lax.dot_general(a, b, (((1,), (0,)), ((), ())), preferred_element_type=F32)


def dot_nt(a, b):
    return lax.dot_general(a, b, (((1,), (1,)), ((), ())), preferred_element_type=F32)


def exact_dot(a_stack, b_parts, product=dot):
    rows = a_stack.shape[0] // 3
    b_hi, b_mid, b_lo = b_parts
    r1 = product(a_stack, b_hi)
    r2 = product(a_stack[: 2 * rows], b_mid)
    r3 = product(a_stack[:rows], b_lo)
    small = r1[2 * rows :] + r2[rows:] + r3
    return r1[:rows] + (r1[rows : 2 * rows] + r2[:rows] + small)


def iota(shape, dim):
    return lax.broadcasted_iota(jnp.int32, shape, dim)


def kernel(inner, hid_h, nw_h, wz_h, wx_h, wbc_h, wdt_h, cx_h, cbc_h, bx_h, bbc_h, dtb_h, al_h, ds_h, gw_h, wo_h,
           out_ref, hid, nw, wz, wx, wbc, wdt, cx, cbc, bx, bbc, dtb, al, ds, gw, wo,
           ubuf, psend, prcv, qbuf, own, hbuf, x0s, q0s, xs, ys, spread, state, gbuf,
           small_sem, hid_sem, w_sem, ps_sem, pr_sem, qs_sem, qr_sem, us_sem, ur_sem):
    me = lax.axis_index("tp")
    core = me % 2
    chip = me // 2
    peer = me + 1 - 2 * core
    cross = (me + 2) % 4
    n_chunks = hid_h.shape[1] // CHUNK
    subs = CHUNK // SUB
    n_subs = n_chunks * subs
    n_piece = wx_h.shape[2] // PIECE
    layers = nw_h.shape[0]
    local = wx_h.shape[2]
    half = wo_h.shape[2] // 2

    barrier = pltpu.get_barrier_semaphore()
    for other in (peer, cross):
        pl.semaphore_signal(barrier, inc=1, device_id={"tp": other}, device_id_type=MESH)

    smalls = [pltpu.make_async_copy(src, dst, small_sem.at[i]) for i, (src, dst) in enumerate(
        [(nw_h, nw), (cx_h, cx), (cbc_h, cbc), (bx_h, bx), (bbc_h, bbc), (dtb_h, dtb), (al_h, al), (ds_h, ds), (gw_h, gw), (wdt_h, wdt)])]

    def hid_copy(c):
        return pltpu.make_async_copy(hid_h.at[0, pl.ds(c * SUB, SUB)], hid.at[c], hid_sem.at[c])

    def weight_copies(layer):
        cols = lambda n: pl.ds(n * PIECE, PIECE)
        bc = pltpu.make_async_copy(wbc_h.at[layer], wbc.at[layer], w_sem.at[layer, 0])
        xcp = [pltpu.make_async_copy(wx_h.at[layer, :, cols(n)], wx.at[layer, n], w_sem.at[layer, 1 + n]) for n in range(n_piece)]
        zcp = [pltpu.make_async_copy(wz_h.at[layer, :, cols(n)], wz.at[layer, n], w_sem.at[layer, 5 + n]) for n in range(n_piece)]
        ocp = []
        for side in range(2):
            for n in range(n_piece):
                ocp.append(pltpu.make_async_copy(wo_h.at[layer, :, cols(side * n_piece + n)], wo.at[layer, side, n], w_sem.at[layer, 9 + side * n_piece + n]))
        return bc, xcp, zcp, ocp

    for r in range(subs):
        hid_copy(r).start()
    for cp in smalls:
        cp.start()
    bc_cp, x_cp, z_cp, o_cp = weight_copies(0)
    bc_cp.start()
    x_cp[0].start()
    x_cp[1].start()
    for r in range(subs, n_subs):
        hid_copy(r).start()

    def rows_of(m):
        return SUB + EXTRA if m == 0 else SUB

    def p_copy(s, m):
        part = pl.ds(0, rows_of(m))
        return pltpu.make_async_remote_copy(src_ref=psend.at[s, m, part], dst_ref=prcv.at[s, m, part], send_sem=ps_sem.at[s, m],
                                            recv_sem=pr_sem.at[s, m], device_id={"tp": peer}, device_id_type=MESH)

    def q_copy(s, m):
        part = pl.ds(0, rows_of(m))
        return pltpu.make_async_remote_copy(src_ref=qbuf.at[chip, s, m, part], dst_ref=qbuf.at[chip, s, m, part], send_sem=qs_sem.at[s, m],
                                            recv_sem=qr_sem.at[s, m], device_id={"tp": cross}, device_id_type=MESH)

    def u_copy(s, m):
        layer, c = s // n_subs, s % n_subs
        return pltpu.make_async_remote_copy(src_ref=ubuf.at[layer + 1, core, c, m], dst_ref=ubuf.at[layer + 1, core, c, m], send_sem=us_sem.at[s, m],
                                            recv_sem=ur_sem.at[s, m], device_id={"tp": peer}, device_id_type=MESH)

    row64 = iota((SUB, PIECE), 0)
    lane64 = iota((SUB, PIECE), 1) % HEAD
    eye = row64 == lane64
    causal = row64 >= lane64
    low_head = iota((SUB, 128), 1) < HEAD

    def to_row(col):
        return jnp.sum(jnp.where(eye, col, 0.0), axis=0, keepdims=True)

    def to_col(row):
        return jnp.sum(jnp.where(eye[:, :HEAD], row[:, :HEAD], 0.0), axis=1, keepdims=True)

    def scale_of(square_sum):
        return lax.rsqrt(square_sum / inner + EPSILON) * (1.0 / 64.0)

    def inverse_of(square_sum):
        return jnp.where(square_sum < jnp.inf, 64.0 * jnp.sqrt(square_sum / inner + EPSILON), 0.0)

    def head_blocks(part):
        left, right = part[:, :128], part[:, 128:]
        none = jnp.zeros_like(left)
        rows = [jnp.concatenate([jnp.where(low_head, left, 0.0), none], axis=1), jnp.concatenate([jnp.where(low_head, 0.0, left), none], axis=1),
                jnp.concatenate([none, jnp.where(low_head, right, 0.0)], axis=1), jnp.concatenate([none, jnp.where(low_head, 0.0, right)], axis=1)]
        return jnp.concatenate(rows, axis=0).astype(BF16)

    def row_of(ref, layer, lanes=slice(None)):
        row = ref[0:1, lanes]
        for at in range(1, layers):
            row = jnp.where(layer == at, ref[at : at + 1, lanes], row)
        return row.astype(F32)

    def start_layer():
        state[...] = jnp.zeros_like(state)
        x0s[0:8] = jnp.zeros((8, local), F32)
        q0s[0:8] = jnp.zeros((8, q0s.shape[1]), F32)

    def tap_sum(buf, lanes, kern, bias):
        total = bias
        for j in range(4):
            total = total + buf[5 + j : 5 + j + CHUNK, lanes] * kern[j : j + 1].astype(F32)
        return total

    def head(layer, c, first):
        square = [jnp.zeros((SUB, 1), F32) for _ in range(subs)]
        for r in range(subs):
            for side in range(2):
                for m in range(n_piece):
                    val = ubuf[layer, side, subs * c + r, m]
                    square[r] = square[r] + jnp.sum(val * val, axis=1, keepdims=True)
        norm_row = row_of(nw, layer)
        for r in range(subs):
            scale = lax.rsqrt(square[r] / (2 * half) + EPSILON)
            for side in range(2):
                for m in range(n_piece):
                    at = side * half + m * PIECE
                    hbuf[r * SUB : (r + 1) * SUB, at : at + PIECE] = (ubuf[layer, side, subs * c + r, m] * scale * norm_row[:, at : at + PIECE]).astype(BF16)
        if first:
            bc_cp.wait()
            x_cp[2].start()
            x_cp[3].start()
        q0s[8:, :] = dot(hbuf[...], wbc[layer]).astype(BF16).astype(F32)
        wdt3 = jnp.concatenate([wdt[layer]] * 3, axis=0)
        r_pre = dot_nt(hbuf[...], wdt3).astype(BF16).astype(F32)
        for n in range(n_piece):
            at = slice(n * PIECE, (n + 1) * PIECE)
            if first and n % 2 == 0:
                x_cp[n].wait()
                x_cp[n + 1].wait()
                for cp in z_cp if n == 0 else o_cp:
                    cp.start()
            x0s[8:, at] = dot(hbuf[...], wx[layer, n]).astype(BF16).astype(F32)
        bc = jax.nn.silu(tap_sum(q0s, slice(None), cbc[layer], row_of(bbc, layer)))
        q0s[0:8] = q0s[CHUNK : CHUNK + 8]
        triple = lambda ref: jnp.concatenate([row_of(ref, layer)] * 3, axis=1)
        dt_in = r_pre + triple(dtb)
        dt_val = jnp.maximum(dt_in, 0.0) + jnp.log1p(jnp.exp(-jnp.abs(dt_in)))
        a_vals = -dt_val * jnp.exp(triple(al))
        to_t, from_t = iota((CHUNK, 3 * CHUNK), 0), iota((CHUNK, 3 * CHUNK), 1) % CHUNK
        tri = jnp.where((to_t >= from_t) & (to_t // SUB == from_t // SUB), 1.0, 0.0).astype(BF16)
        a_cum = dot(tri, stack3(a_vals))
        skip = jnp.broadcast_to(triple(ds), (8, a_cum.shape[1]))
        to_spread = jnp.concatenate([dt_val, a_cum, skip], axis=0)
        hi, mid, lo = split3(to_spread)
        lane = iota(to_spread.shape, 1)
        n_heads = local // HEAD
        spread_in = jnp.where(lane < n_heads, hi, jnp.where(lane < 2 * n_heads, mid, lo)).astype(BF16)
        for n in range(n_piece):
            at = slice(n * PIECE, (n + 1) * PIECE)
            group = n * (PIECE // HEAD)
            pick = jnp.where(iota((3 * n_heads, PIECE), 1) // HEAD + group == iota((3 * n_heads, PIECE), 0) % n_heads, 1.0, 0.0).astype(BF16)
            spread[:, at] = dot(spread_in, pick)
        swapped = pltpu.roll(bc, HEAD, 1)
        turned = jnp.transpose(bc)
        c_stack, bt_stack, cb = [], [], []
        for r in range(subs):
            rows = slice(r * SUB, (r + 1) * SUB)
            c_stack.append(stack3(swapped[rows, :HEAD]))
            bt_stack.append(stack3(turned[:HEAD, rows]))
            cb.append(exact_dot(c_stack[r], [jnp.concatenate([part] * 4, axis=0).astype(BF16) for part in split3(bc[rows, :HEAD])], dot_nt))
        for n in range(n_piece):
            at = slice(n * PIECE, (n + 1) * PIECE)
            xs[:, at] = jax.nn.silu(tap_sum(x0s, at, cx[layer, :, at], row_of(bx, layer, at)))
            x0s[0:8, at] = x0s[CHUNK : CHUNK + 8, at]
        for r in range(subs):
            rows = slice(r * SUB, (r + 1) * SUB)
            for n in range(n_piece):
                at = slice(n * PIECE, (n + 1) * PIECE)
                a_e = spread[CHUNK + r * SUB : CHUNK + (r + 1) * SUB, at]
                decay = jnp.where(causal, jnp.exp(jnp.minimum(a_e - to_row(a_e), 0.0)), 0.0) * cb[r]
                x_dt = xs[rows, at] * spread[rows, at]
                ys[rows, at] = exact_dot(stack3(decay), [head_blocks(part) for part in split3(x_dt)])
        for r in range(subs):
            rows = slice(r * SUB, (r + 1) * SUB)
            for n in range(n_piece):
                at = slice(n * PIECE, (n + 1) * PIECE)
                a_e = spread[CHUNK + r * SUB : CHUNK + (r + 1) * SUB, at]
                a_last = a_e[SUB - 1 : SUB]
                old = state[:, at]
                carried = exact_dot(c_stack[r], [part.astype(BF16) for part in split3(old)])
                x_act = xs[rows, at]
                ys[rows, at] = ys[rows, at] + carried * jnp.exp(a_e) + spread[2 * CHUNK : 2 * CHUNK + 1, at] * x_act
                tail_x = x_act * spread[rows, at] * jnp.exp(a_last - a_e)
                state[:, at] = jnp.exp(a_last) * old + exact_dot(bt_stack[r], [part.astype(BF16) for part in split3(tail_x)])

    def tail(layer, c, first):
        s = (layer * n_chunks + c) * subs
        gate_sq = jnp.zeros((CHUNK, 1), F32)
        if first:
            for cp in z_cp:
                cp.wait()
        for n in range(n_piece):
            at = slice(n * PIECE, (n + 1) * PIECE)
            z = dot(hbuf[...], wz[layer, n]).astype(BF16).astype(F32)
            v = ys[:, at] * jax.nn.silu(z)
            ys[:, at] = v
            gate_sq = gate_sq + jnp.sum(v * v, axis=1, keepdims=True)
        scale = scale_of(gate_sq)
        gbuf[...] = (ys[...] * scale * row_of(gw, layer)).astype(BF16)
        for r in range(subs):
            psend[s + r, 0, SUB:] = jnp.broadcast_to(to_row(gate_sq[r * SUB : (r + 1) * SUB]), (EXTRA, PIECE))
        if first:
            for cp in o_cp:
                cp.wait()
        for m in range(n_piece):
            part = dot(gbuf[...], wo[layer, 1 - core, m])
            for r in range(subs):
                psend[s + r, m, 0:SUB] = part[r * SUB : (r + 1) * SUB]
        if first:
            pl.semaphore_wait(barrier, 2)
        for r in range(subs):
            for m in range(n_piece):
                p_copy(s + r, m).start()
        for m in range(n_piece):
            part = dot(gbuf[...], wo[layer, core, m])
            for r in range(subs):
                own[r, m] = part[r * SUB : (r + 1) * SUB]

    def combine(s):
        for m in range(n_piece):
            p_copy(s, m).wait_recv()
            if m == 0:
                own_sq = to_col(psend[s, 0, SUB : SUB + 1])
                peer_sq = to_col(prcv[s, 0, SUB : SUB + 1])
                chip_sq = own_sq + peer_sq
                chip_scale = scale_of(chip_sq)
                f_own = chip_scale * inverse_of(own_sq)
                f_peer = chip_scale * inverse_of(peer_sq)
                qbuf[chip, s, 0, SUB:] = jnp.broadcast_to(to_row(chip_sq), (EXTRA, PIECE))
            qbuf[chip, s, m, 0:SUB] = own[s % subs, m] * f_own + prcv[s, m, 0:SUB] * f_peer
            q_copy(s, m).start()

    def update(s):
        layer, c = s // n_subs, s % n_subs
        for m in range(n_piece):
            q_copy(s, m).wait_recv()
            if m == 0:
                sq0 = to_col(qbuf[0, s, 0, SUB : SUB + 1])
                sq1 = to_col(qbuf[1, s, 0, SUB : SUB + 1])
                norm = lax.rsqrt((sq0 + sq1) / inner + EPSILON)
                f0 = norm * inverse_of(sq0)
                f1 = norm * inverse_of(sq1)
            total = ubuf[layer, core, c, m] + (qbuf[0, s, m, 0:SUB] * f0 + qbuf[1, s, m, 0:SUB] * f1)
            ubuf[layer + 1, core, c, m] = total.astype(BF16).astype(F32)
            u_copy(s, m).start()

    def emit(s):
        c = s % n_subs
        for side in (core, 1 - core):
            for m in range(n_piece):
                if side is not core:
                    u_copy(s, m).wait_recv()
                cols = pl.ds(pl.multiple_of(side * half + m * PIECE, PIECE), PIECE)
                out_ref[0, pl.ds(pl.multiple_of(c * SUB, SUB), SUB), cols] = ubuf[layers, side, c, m].astype(BF16)

    def load_hidden(c):
        hid_copy(c).wait()
        for side in range(2):
            for m in range(n_piece):
                at = side * half + m * PIECE
                ubuf[0, side, c, m] = hid[c, :, at : at + PIECE].astype(F32)

    start_layer()
    for r in range(subs):
        load_hidden(r)
    for cp in smalls:
        cp.wait()
    head(0, 0, True)
    tail(0, 0, True)
    later = [weight_copies(layer) for layer in range(1, layers)]
    for groups in later:
        groups[0].start()
        for group in groups[1:]:
            for cp in group:
                cp.start()
    for r in range(subs):
        combine(r)

    @pl.loop(1, layers * n_chunks)
    def _(t):
        layer, c = t // n_chunks, t % n_chunks
        for at in range(1, layers):
            @pl.when(t == at * n_chunks)
            def _():
                start_layer()
                later[at - 1][0].wait()
                for group in later[at - 1][1:]:
                    for cp in group:
                        cp.wait()

        @pl.when(t < n_chunks)
        def _():
            for r in range(subs):
                load_hidden(c * subs + r)

        @pl.when(t >= n_chunks)
        def _():
            before = (t - n_chunks) * subs
            for r in range(subs):
                update(before + r)
            for r in range(subs):
                for m in range(n_piece):
                    u_copy(before + r, m).wait_recv()

        head(layer, c, False)
        tail(layer, c, False)
        for r in range(subs):
            combine(t * subs + r)

    @pl.loop((layers - 1) * n_subs, layers * n_subs)
    def _(s):
        update(s)

    @pl.loop((layers - 1) * n_subs, layers * n_subs)
    def _(s):
        emit(s)

    @pl.loop(0, layers * n_subs)
    def _(s):
        for m in range(n_piece):
            p_copy(s, m).wait_send()
            q_copy(s, m).wait_send()
            u_copy(s, m).wait_send()


def solution(mesh):
    in_specs = (P('dp'), P(), P(None, None, 'tp'), P(None, None, 'tp'), P(), P(None, None, 'tp'), P(None, None, 'tp'), P(), P(None, 'tp'), P(),
                P(None, 'tp'), P(None, 'tp'), P(None, 'tp'), P(None, 'tp'), P(None, 'tp', None))
    tp_size = mesh.shape['tp']

    def device_forward(hidden, norm_w, w_z, w_x, w_bc, w_dt, conv_x, conv_bc, bias_x, bias_bc, dt_bias, a_log, d_skip, gate_w, w_out):
        layers, width, local = w_x.shape
        n_subs = hidden.shape[1] // SUB
        n_piece = local // PIECE
        steps = layers * n_subs
        bc_width = w_bc.shape[-1]
        w_dt = jnp.swapaxes(w_dt, 1, 2)
        vm = lambda shape, dtype: pltpu.VMEM(shape, dtype)
        same = lambda arr: pltpu.VMEM(arr.shape, arr.dtype)
        scratch = [
            vm((n_subs, SUB, width), BF16), same(norm_w), vm((layers, n_piece, width, PIECE), BF16), vm((layers, n_piece, width, PIECE), BF16),
            same(w_bc), same(w_dt), same(conv_x), same(conv_bc), same(bias_x), same(bias_bc), same(dt_bias), same(a_log), same(d_skip), same(gate_w),
            vm((layers, 2, n_piece, local, PIECE), BF16),
            vm((layers + 1, 2, n_subs, n_piece, SUB, PIECE), F32),
            vm((steps, n_piece, SUB + EXTRA, PIECE), F32), vm((steps, n_piece, SUB + EXTRA, PIECE), F32),
            vm((2, steps, n_piece, SUB + EXTRA, PIECE), F32),
            vm((CHUNK // SUB, n_piece, SUB, PIECE), F32), vm((CHUNK, width), BF16), vm((CHUNK + 8, local), F32), vm((CHUNK + 8, bc_width), F32),
            vm((CHUNK, local), F32), vm((CHUNK, local), F32), vm((2 * CHUNK + 8, local), F32), vm((HEAD, local), F32), vm((CHUNK, local), BF16),
            pltpu.SemaphoreType.DMA((10,)), pltpu.SemaphoreType.DMA((n_subs,)), pltpu.SemaphoreType.DMA((layers, 9 + 2 * n_piece)),
        ] + [pltpu.SemaphoreType.DMA((steps, n_piece)) for _ in range(6)]
        return pl.pallas_call(
            functools.partial(kernel, float(local * tp_size)),
            out_shape=jax.ShapeDtypeStruct(hidden.shape, hidden.dtype),
            in_specs=[pl.BlockSpec(memory_space=pltpu.HBM)] * 15,
            out_specs=pl.BlockSpec(memory_space=pltpu.VMEM),
            scratch_shapes=scratch,
            compiler_params=pltpu.CompilerParams(collective_id=0, has_side_effects=True, vmem_limit_bytes=52 * 1024 * 1024),
        )(*[pltpu.with_memory_space_constraint(arr, pltpu.HBM) for arr in (hidden, norm_w, w_z, w_x, w_bc, w_dt, conv_x, conv_bc, bias_x, bias_bc, dt_bias, a_log, d_skip, gate_w, w_out)])

    return jax.shard_map(device_forward, mesh=mesh, in_specs=in_specs, out_specs=P('dp'), check_vma=False)
```

```python
import functools

import jax
import jax.numpy as jnp
from jax import lax
from jax.experimental import pallas as pl
from jax.experimental.pallas import tpu as pltpu
from jax.sharding import PartitionSpec as P

EPSILON = 1e-5
MESH = pl.DeviceIdType.MESH
SUB = 64
MAX_ROWS = 64
PIECE = 256
HEAD = 64
F32 = jnp.float32
BF16 = jnp.bfloat16


def split3(val):
    hi = val.astype(BF16).astype(F32)
    rest = val - hi
    mid = rest.astype(BF16).astype(F32)
    return hi, mid, rest - mid


def stack3(val):
    return jnp.concatenate(split3(val), axis=0).astype(BF16)


def dot(a, b):
    return lax.dot_general(a, b, (((1,), (0,)), ((), ())), preferred_element_type=F32)


def dot_nt(a, b):
    return lax.dot_general(a, b, (((1,), (1,)), ((), ())), preferred_element_type=F32)


def exact_dot(a_stack, b_parts, product=dot):
    rows = a_stack.shape[0] // 3
    b_hi, b_mid, b_lo = b_parts
    r1 = product(a_stack, b_hi)
    r2 = product(a_stack[: 2 * rows], b_mid)
    r3 = product(a_stack[:rows], b_lo)
    small = r1[2 * rows :] + r2[rows:] + r3
    return r1[:rows] + (r1[rows : 2 * rows] + r2[:rows] + small)


def iota(shape, dim):
    return lax.broadcasted_iota(jnp.int32, shape, dim)


def kernel(inner, hid_h, nw_h, wz_h, wx_h, wbc_h, wdt_h, cx_h, cbc_h, bx_h, bbc_h, dtb_h, al_h, ds_h, gw_h, wo_h,
           out_ref, hid, nw, wz, wx, wbc, wdt, cx, cbc, bx, bbc, dtb, al, ds, gw, wo,
           ubuf, psend, prcv, qbuf, pstat, qstat, own, hbuf, x0s, q0s, xs, ys, spread, state, gbuf,
           small_sem, hid_sem, w_sem, send_sem, pr_sem, qr_sem, ur_sem, ptr_sem, qtr_sem):
    me = lax.axis_index("tp")
    core = me % 2
    chip = me // 2
    peer = me + 1 - 2 * core
    cross = (me + 2) % 4
    n_subs = hid_h.shape[1] // SUB
    n_piece = wx_h.shape[2] // PIECE
    layers = nw_h.shape[0]
    local = wx_h.shape[2]
    half = wo_h.shape[2] // 2

    barrier = pltpu.get_barrier_semaphore()
    for other in (peer, cross):
        pl.semaphore_signal(barrier, inc=1, device_id={"tp": other}, device_id_type=MESH)

    smalls = [pltpu.make_async_copy(src, dst, small_sem.at[i]) for i, (src, dst) in enumerate(
        [(nw_h, nw), (cx_h, cx), (cbc_h, cbc), (bx_h, bx), (bbc_h, bbc), (dtb_h, dtb), (al_h, al), (ds_h, ds), (gw_h, gw), (wdt_h, wdt)])]

    def hid_copy(c):
        return pltpu.make_async_copy(hid_h.at[0, pl.ds(c * SUB, SUB)], hid.at[c], hid_sem.at[c])

    def weight_copies(layer):
        cols = lambda n: pl.ds(n * PIECE, PIECE)
        bc = pltpu.make_async_copy(wbc_h.at[layer], wbc.at[layer], w_sem.at[0])
        xcp = [pltpu.make_async_copy(wx_h.at[layer, :, cols(n)], wx.at[layer, n], w_sem.at[1 + n // 2]) for n in range(n_piece)]
        zcp = [pltpu.make_async_copy(wz_h.at[layer, :, cols(n)], wz.at[layer, n], w_sem.at[3]) for n in range(n_piece)]
        ocp = []
        for n in range(n_piece):
            for side in range(2):
                ocp.append(pltpu.make_async_copy(wo_h.at[layer, :, cols(side * n_piece + n)], wo.at[layer, side, n], w_sem.at[4]))
        return bc, xcp, zcp, ocp

    def weight_waits(layer):
        whole = lambda ref, sem: pltpu.make_async_copy(ref, ref, w_sem.at[sem])
        return [whole(wbc.at[layer], 0), whole(wx.at[layer, pl.ds(0, 2)], 1), whole(wx.at[layer, pl.ds(2, 2)], 2), whole(wz.at[layer], 3), whole(wo.at[layer], 4)]

    bc_cp, x_cp, z_cp, o_cp = weight_copies(0)
    first_wait = weight_waits(0)
    hid_copy(0).start()
    smalls[0].start()
    bc_cp.start()
    x_cp[0].start()
    x_cp[1].start()

    def remote(src, dst, sem, recv_sem, target):
        return pltpu.make_async_remote_copy(src_ref=src, dst_ref=dst, send_sem=send_sem.at[sem], recv_sem=recv_sem, device_id={"tp": target}, device_id_type=MESH)

    last = layers * n_subs - 1

    def own_slot(s, m):
        return s + m * (s // last)

    def p_copy(s, m):
        return remote(psend.at[s, m], prcv.at[s, m], 0, pr_sem.at[s % 2, m], peer)

    def pstat_copy(s):
        return remote(pstat.at[core, s], pstat.at[core, s], 1, ptr_sem.at[s % 2], peer)

    def q_copy(s, m):
        return remote(qbuf.at[chip, s, m], qbuf.at[chip, s, m], 2, qr_sem.at[own_slot(s, m)], cross)

    def qstat_copy(s):
        return remote(qstat.at[chip, s], qstat.at[chip, s], 3, qtr_sem.at[s], cross)

    def u_copy(s, m):
        spot = ubuf.at[s // n_subs + 1, core, s % n_subs, m]
        return remote(spot, spot, 4, ur_sem.at[own_slot(s, m)], peer)

    def q_arrived(s):
        remote(qbuf.at[chip, s], qbuf.at[chip, s], 2, qr_sem.at[s], cross).wait_recv()

    def u_arrived(s):
        spot = ubuf.at[s // n_subs + 1, core, s % n_subs]
        remote(spot, spot, 4, ur_sem.at[s], peer).wait_recv()

    def all_sent():
        shared = ubuf.at[pl.ds(1, layers), core]
        for sem, ref in enumerate((psend, pstat.at[core], qbuf.at[chip], qstat.at[chip], shared)):
            remote(ref, ref, sem, qtr_sem.at[0], cross).wait_send()

    row64 = iota((SUB, PIECE), 0)
    lane64 = iota((SUB, PIECE), 1) % HEAD
    eye = row64 == lane64
    causal = row64 >= lane64
    low_head = iota((SUB, 128), 1) < HEAD

    def to_row(col):
        return jnp.sum(jnp.where(eye, col, 0.0), axis=0, keepdims=True)

    def to_col(row):
        return jnp.sum(jnp.where(eye[:, :HEAD], row[:, :HEAD], 0.0), axis=1, keepdims=True)

    def scale_of(square_sum):
        return lax.rsqrt(square_sum / inner + EPSILON) * (1.0 / 64.0)

    def inverse_of(square_sum):
        return jnp.where(square_sum < jnp.inf, 64.0 * jnp.sqrt(square_sum / inner + EPSILON), 0.0)

    def head_blocks(part):
        left, right = part[:, :128], part[:, 128:]
        none = jnp.zeros_like(left)
        rows = [jnp.concatenate([jnp.where(low_head, left, 0.0), none], axis=1), jnp.concatenate([jnp.where(low_head, 0.0, left), none], axis=1),
                jnp.concatenate([none, jnp.where(low_head, right, 0.0)], axis=1), jnp.concatenate([none, jnp.where(low_head, 0.0, right)], axis=1)]
        return jnp.concatenate(rows, axis=0).astype(BF16)

    def row_of(ref, layer, lanes=slice(None)):
        row = ref[0:1, lanes]
        for at in range(1, layers):
            row = jnp.where(layer == at, ref[at : at + 1, lanes], row)
        return row.astype(F32)

    def start_layer():
        state[...] = jnp.zeros_like(state)
        x0s[0:8] = jnp.zeros((8, local), F32)
        q0s[0:8] = jnp.zeros((8, q0s.shape[1]), F32)

    def tap_sum(buf, size, lanes, kern, bias):
        total = bias
        for j in range(4):
            total = total + buf[5 + j : 5 + j + size, lanes] * kern[j : j + 1].astype(F32)
        return total

    def norm(layer, q, subs):
        square = [jnp.zeros((SUB, 1), F32) for _ in range(subs)]
        for r in range(subs):
            for side in range(2):
                for m in range(n_piece):
                    val = ubuf[layer, side, q + r, m]
                    square[r] = square[r] + jnp.sum(val * val, axis=1, keepdims=True)
        norm_row = row_of(nw, layer)
        for r in range(subs):
            scale = lax.rsqrt(square[r] / (2 * half) + EPSILON)
            for side in range(2):
                for m in range(n_piece):
                    at = side * half + m * PIECE
                    hbuf[r * SUB : (r + 1) * SUB, at : at + PIECE] = (ubuf[layer, side, q + r, m] * scale * norm_row[:, at : at + PIECE]).astype(BF16)

    def head(layer, q, subs, first, hook):
        size = subs * SUB
        if first:
            first_wait[0].wait()
            smalls[-1].wait()
        q0s[8 : 8 + size, :] = dot(hbuf[:size], wbc[layer]).astype(BF16).astype(F32)
        wdt3 = jnp.concatenate([wdt[layer]] * 3, axis=0)
        r_pre = dot_nt(hbuf[:size], wdt3).astype(BF16).astype(F32)
        for n in range(n_piece):
            at = slice(n * PIECE, (n + 1) * PIECE)
            if first and n % 2 == 0:
                first_wait[1 + n // 2].wait()
            x0s[8 : 8 + size, at] = dot(hbuf[:size], wx[layer, n]).astype(BF16).astype(F32)
        hook()
        if first:
            for cp in smalls[1:-1]:
                cp.wait()
            for cp in o_cp:
                cp.start()
        bc = jax.nn.silu(tap_sum(q0s, size, slice(None), cbc[layer], row_of(bbc, layer)))
        q0s[0:8] = q0s[size : size + 8]
        triple = lambda ref: jnp.concatenate([row_of(ref, layer)] * 3, axis=1)
        dt_in = r_pre + triple(dtb)
        dt_val = jnp.maximum(dt_in, 0.0) + jnp.log1p(jnp.exp(-jnp.abs(dt_in)))
        a_vals = -dt_val * jnp.exp(triple(al))
        to_t, from_t = iota((size, 3 * size), 0), iota((size, 3 * size), 1) % size
        tri = jnp.where((to_t >= from_t) & (to_t // SUB == from_t // SUB), 1.0, 0.0).astype(BF16)
        a_cum = dot(tri, stack3(a_vals))
        skip = jnp.broadcast_to(triple(ds), (8, a_cum.shape[1]))
        to_spread = jnp.concatenate([dt_val, a_cum, skip], axis=0)
        hi, mid, lo = split3(to_spread)
        lane = iota(to_spread.shape, 1)
        n_heads = local // HEAD
        spread_in = jnp.where(lane < n_heads, hi, jnp.where(lane < 2 * n_heads, mid, lo)).astype(BF16)
        for n in range(n_piece):
            at = slice(n * PIECE, (n + 1) * PIECE)
            group = n * (PIECE // HEAD)
            pick = jnp.where(iota((3 * n_heads, PIECE), 1) // HEAD + group == iota((3 * n_heads, PIECE), 0) % n_heads, 1.0, 0.0).astype(BF16)
            spread[: 2 * size + 8, at] = dot(spread_in, pick)
        swapped = pltpu.roll(bc, HEAD, 1)
        turned = jnp.transpose(bc)
        c_stack, bt_stack, cb = [], [], []
        for r in range(subs):
            rows = slice(r * SUB, (r + 1) * SUB)
            c_stack.append(stack3(swapped[rows, :HEAD]))
            bt_stack.append(stack3(turned[:HEAD, rows]))
            cb.append(exact_dot(c_stack[r], [jnp.concatenate([part] * 4, axis=0).astype(BF16) for part in split3(bc[rows, :HEAD])], dot_nt))
        for n in range(n_piece):
            at = slice(n * PIECE, (n + 1) * PIECE)
            xs[:size, at] = jax.nn.silu(tap_sum(x0s, size, at, cx[layer, :, at], row_of(bx, layer, at)))
            x0s[0:8, at] = x0s[size : size + 8, at]
        for r in range(subs):
            rows = slice(r * SUB, (r + 1) * SUB)
            for n in range(n_piece):
                at = slice(n * PIECE, (n + 1) * PIECE)
                a_e = spread[size + r * SUB : size + (r + 1) * SUB, at]
                decay = jnp.where(causal, jnp.exp(jnp.minimum(a_e - to_row(a_e), 0.0)), 0.0) * cb[r]
                x_dt = xs[rows, at] * spread[rows, at]
                ys[rows, at] = exact_dot(stack3(decay), [head_blocks(part) for part in split3(x_dt)])
        for r in range(subs):
            rows = slice(r * SUB, (r + 1) * SUB)
            for n in range(n_piece):
                at = slice(n * PIECE, (n + 1) * PIECE)
                a_e = spread[size + r * SUB : size + (r + 1) * SUB, at]
                a_last = a_e[SUB - 1 : SUB]
                old = state[:, at]
                carried = exact_dot(c_stack[r], [part.astype(BF16) for part in split3(old)])
                x_act = xs[rows, at]
                ys[rows, at] = ys[rows, at] + carried * jnp.exp(a_e) + spread[2 * size : 2 * size + 1, at] * x_act
                tail_x = x_act * spread[rows, at] * jnp.exp(a_last - a_e)
                state[:, at] = jnp.exp(a_last) * old + exact_dot(bt_stack[r], [part.astype(BF16) for part in split3(tail_x)])

    def tail(layer, q, subs, first):
        size = subs * SUB
        s = layer * n_subs + q
        gate_sq = jnp.zeros((size, 1), F32)
        if first:
            first_wait[3].wait()
        for n in range(n_piece):
            at = slice(n * PIECE, (n + 1) * PIECE)
            z = dot(hbuf[:size], wz[layer, n]).astype(BF16).astype(F32)
            v = ys[:size, at] * jax.nn.silu(z)
            ys[:size, at] = v
            gate_sq = gate_sq + jnp.sum(v * v, axis=1, keepdims=True)
        scale = scale_of(gate_sq)
        gbuf[:size] = (ys[:size] * scale * row_of(gw, layer)).astype(BF16)
        for r in range(subs):
            pstat[core, s + r] = to_row(gate_sq[r * SUB : (r + 1) * SUB])[:, :128]
        if first:
            for q_next in range(1, n_subs):
                hid_copy(q_next).start()
            first_wait[4].wait()
        for m in range(n_piece):
            part = dot(gbuf[:size], wo[layer, 1 - core, m])
            for r in range(subs):
                psend[s + r, m] = part[r * SUB : (r + 1) * SUB]
        if first:
            pl.semaphore_wait(barrier, 2)
        for r in range(subs):
            pstat_copy(s + r).start()
            for m in range(n_piece):
                p_copy(s + r, m).start()
        for m in range(n_piece):
            part = dot(gbuf[:size], wo[layer, core, m])
            for r in range(subs):
                own[m] = part[r * SUB : (r + 1) * SUB]

    def combine(s):
        pstat_copy(s).wait_recv()
        own_sq = to_col(pstat[core, s])
        peer_sq = to_col(pstat[1 - core, s])
        chip_sq = own_sq + peer_sq
        chip_scale = scale_of(chip_sq)
        f_own = chip_scale * inverse_of(own_sq)
        f_peer = chip_scale * inverse_of(peer_sq)
        qstat[chip, s] = to_row(chip_sq)[:, :128]
        qstat_copy(s).start()
        for m in range(n_piece):
            p_copy(s, m).wait_recv()
            qbuf[chip, s, m] = own[m] * f_own + prcv[s, m] * f_peer
            q_copy(s, m).start()

    def update(s, pieces=False):
        layer, c = s // n_subs, s % n_subs
        qstat_copy(s).wait_recv()
        if not pieces:
            q_arrived(s)
        sq0 = to_col(qstat[0, s])
        sq1 = to_col(qstat[1, s])
        norm = lax.rsqrt((sq0 + sq1) / inner + EPSILON)
        f0 = norm * inverse_of(sq0)
        f1 = norm * inverse_of(sq1)
        for m in range(n_piece):
            if pieces:
                q_copy(s, m).wait_recv()
            total = ubuf[layer, core, c, m] + (qbuf[0, s, m] * f0 + qbuf[1, s, m] * f1)
            ubuf[layer + 1, core, c, m] = total.astype(BF16).astype(F32)
            u_copy(s, m).start()

    def emit(s, pieces=False):
        c = s % n_subs
        for side in (core, 1 - core):
            if side is not core and not pieces:
                u_arrived(s)
            for m in range(n_piece):
                if side is not core and pieces:
                    u_copy(s, m).wait_recv()
                cols = pl.ds(pl.multiple_of(side * half + m * PIECE, PIECE), PIECE)
                out_ref[0, pl.ds(pl.multiple_of(c * SUB, SUB), SUB), cols] = ubuf[layers, side, c, m].astype(BF16)

    def load_hidden(c):
        hid_copy(c).wait()
        for side in range(2):
            for m in range(n_piece):
                at = side * half + m * PIECE
                ubuf[0, side, c, m] = hid[c, :, at : at + PIECE].astype(F32)

    steps = layers * n_subs
    lag = n_subs - 1
    steps = layers * n_subs
    lag = n_subs - 1
    start_layer()
    load_hidden(0)
    for cp in x_cp[2:] + smalls[-1:] + smalls[1:-1] + z_cp:
        cp.start()
    smalls[0].wait()
    norm(0, 0, 1)
    head(0, 0, 1, True, lambda: None)
    tail(0, 0, 1, True)

    def start_weights(layer):
        bc_cp, x_cp, z_cp, o_cp = weight_copies(layer)
        for cp in [bc_cp] + x_cp + z_cp + o_cp:
            cp.start()

    start_weights(1)
    combine(0)

    @pl.loop(1, steps)
    def _(t):
        layer, q = t // n_subs, t % n_subs

        @pl.when(t < n_subs)
        def _():
            load_hidden(q)

        @pl.when(t >= n_subs)
        def _():
            u_arrived(t - n_subs)

        for at in range(1, layers):
            @pl.when(t == at * n_subs)
            def _():
                start_layer()
                for cp in weight_waits(at):
                    cp.wait()
                if at + 1 < layers:
                    start_weights(at + 1)

        norm(layer, q, 1)

        @pl.when(t >= lag)
        def _():
            update(t - lag)

        def hook():
            @pl.when(t >= 2)
            def _():
                combine(t - 1)

        head(layer, q, 1, False, hook)
        tail(layer, q, 1, False)

    combine(steps - 1)
    final = steps - n_subs

    @pl.loop(final, steps - 1)
    def _(s):
        @pl.when(s > final)
        def _():
            emit(s - 1)

        @pl.when(s > steps - 1 - lag)
        def _():
            update(s)

    emit(steps - 2)
    update(steps - 1, True)
    emit(steps - 1, True)
    all_sent()


def solution(mesh):
    in_specs = (P('dp'), P(), P(None, None, 'tp'), P(None, None, 'tp'), P(), P(None, None, 'tp'), P(None, None, 'tp'), P(), P(None, 'tp'), P(),
                P(None, 'tp'), P(None, 'tp'), P(None, 'tp'), P(None, 'tp'), P(None, 'tp', None))
    tp_size = mesh.shape['tp']

    def device_forward(hidden, norm_w, w_z, w_x, w_bc, w_dt, conv_x, conv_bc, bias_x, bias_bc, dt_bias, a_log, d_skip, gate_w, w_out):
        layers, width, local = w_x.shape
        n_subs = hidden.shape[1] // SUB
        n_piece = local // PIECE
        steps = layers * n_subs
        bc_width = w_bc.shape[-1]
        w_dt = jnp.swapaxes(w_dt, 1, 2)
        vm = lambda shape, dtype: pltpu.VMEM(shape, dtype)
        same = lambda arr: pltpu.VMEM(arr.shape, arr.dtype)
        scratch = [
            vm((n_subs, SUB, width), BF16), same(norm_w), vm((layers, n_piece, width, PIECE), BF16), vm((layers, n_piece, width, PIECE), BF16),
            same(w_bc), same(w_dt), same(conv_x), same(conv_bc), same(bias_x), same(bias_bc), same(dt_bias), same(a_log), same(d_skip), same(gate_w),
            vm((layers, 2, n_piece, local, PIECE), BF16),
            vm((layers + 1, 2, n_subs, n_piece, SUB, PIECE), F32),
            vm((steps, n_piece, SUB, PIECE), F32), vm((steps, n_piece, SUB, PIECE), F32), vm((2, steps, n_piece, SUB, PIECE), F32),
            vm((2, steps, 1, 128), F32), vm((2, steps, 1, 128), F32),
            vm((n_piece, SUB, PIECE), F32), vm((MAX_ROWS, width), BF16), vm((MAX_ROWS + 8, local), F32), vm((MAX_ROWS + 8, bc_width), F32),
            vm((MAX_ROWS, local), F32), vm((MAX_ROWS, local), F32), vm((2 * MAX_ROWS + 8, local), F32), vm((HEAD, local), F32), vm((MAX_ROWS, local), BF16),
            pltpu.SemaphoreType.DMA((10,)), pltpu.SemaphoreType.DMA((n_subs,)), pltpu.SemaphoreType.DMA((5,)), pltpu.SemaphoreType.DMA((5,)),
            pltpu.SemaphoreType.DMA((2, n_piece)), pltpu.SemaphoreType.DMA((steps - 1 + n_piece,)), pltpu.SemaphoreType.DMA((steps - 1 + n_piece,)),
            pltpu.SemaphoreType.DMA((2,)), pltpu.SemaphoreType.DMA((steps,)),
        ]
        return pl.pallas_call(
            functools.partial(kernel, float(local * tp_size)),
            out_shape=jax.ShapeDtypeStruct(hidden.shape, hidden.dtype),
            in_specs=[pl.BlockSpec(memory_space=pltpu.HBM)] * 15,
            out_specs=pl.BlockSpec(memory_space=pltpu.VMEM),
            scratch_shapes=scratch,
            compiler_params=pltpu.CompilerParams(collective_id=0, has_side_effects=True, vmem_limit_bytes=52 * 1024 * 1024),
        )(*[pltpu.with_memory_space_constraint(arr, pltpu.HBM) for arr in (hidden, norm_w, w_z, w_x, w_bc, w_dt, conv_x, conv_bc, bias_x, bias_bc, dt_bias, a_log, d_skip, gate_w, w_out)])

    return jax.shard_map(device_forward, mesh=mesh, in_specs=in_specs, out_specs=P('dp'), check_vma=False)
```

```python
import functools

import jax
import jax.numpy as jnp
from jax import lax
from jax.experimental import pallas as pl
from jax.experimental.pallas import tpu as pltpu
from jax.sharding import PartitionSpec as P

EPSILON = 1e-5
MESH = pl.DeviceIdType.MESH
SUB = 64
MAX_ROWS = 64
PIECE = 256
HEAD = 64
F32 = jnp.float32
BF16 = jnp.bfloat16


def split3(val):
    hi = val.astype(BF16).astype(F32)
    rest = val - hi
    mid = rest.astype(BF16).astype(F32)
    return hi, mid, rest - mid


def stack3(val):
    return jnp.concatenate(split3(val), axis=0).astype(BF16)


def dot(a, b):
    return lax.dot_general(a, b, (((1,), (0,)), ((), ())), preferred_element_type=F32)


def dot_nt(a, b):
    return lax.dot_general(a, b, (((1,), (1,)), ((), ())), preferred_element_type=F32)


def exact_dot(a_stack, b_parts, product=dot):
    rows = a_stack.shape[0] // 3
    b_hi, b_mid, b_lo = b_parts
    r1 = product(a_stack, b_hi)
    r2 = product(a_stack[: 2 * rows], b_mid)
    r3 = product(a_stack[:rows], b_lo)
    small = r1[2 * rows :] + r2[rows:] + r3
    return r1[:rows] + (r1[rows : 2 * rows] + r2[:rows] + small)


def iota(shape, dim):
    return lax.broadcasted_iota(jnp.int32, shape, dim)


def kernel(inner, hid_h, nw_h, wz_h, wx_h, wbc_h, wdt_h, cx_h, cbc_h, bx_h, bbc_h, dtb_h, al_h, ds_h, gw_h, wo_h,
           out_ref, hid, nw, wz, wx, wbd, wdt, cx, cbc, bx, bbc, dtb, al, ds, gw, wo,
           ubuf, psend, prcv, qbuf, pstat, qstat, own, hbuf, x0s, q0s, xs, ys, zs, spread, state, gbuf,
           small_sem, hid_sem, w_sem, send_sem, pr_sem, qr_sem, ur_sem, ptr_sem, qtr_sem):
    me = lax.axis_index("tp")
    core = me % 2
    chip = me // 2
    peer = me + 1 - 2 * core
    cross = (me + 2) % 4
    n_subs = hid_h.shape[1] // SUB
    n_piece = wx_h.shape[2] // PIECE
    layers = nw_h.shape[0]
    local = wx_h.shape[2]
    half = wo_h.shape[2] // 2

    barrier = pltpu.get_barrier_semaphore()
    for other in (peer, cross):
        pl.semaphore_signal(barrier, inc=1, device_id={"tp": other}, device_id_type=MESH)

    smalls = [pltpu.make_async_copy(src, dst, small_sem.at[i]) for i, (src, dst) in enumerate(
        [(nw_h, nw), (cx_h, cx), (cbc_h, cbc), (bx_h, bx), (bbc_h, bbc), (dtb_h, dtb), (al_h, al), (ds_h, ds), (gw_h, gw), (wdt_h, wdt)])]

    def hid_copy(c):
        return pltpu.make_async_copy(hid_h.at[0, pl.ds(c * SUB, SUB)], hid.at[c], hid_sem.at[c])

    def start_weights(layer, extra=()):
        cols = lambda n: pl.ds(pl.multiple_of(n * PIECE, PIECE), PIECE)

        @pl.loop(0, n_piece)
        def _(n):
            pltpu.make_async_copy(wx_h.at[layer, :, cols(n)], wx.at[layer, n], w_sem.at[1 + n // 2]).start()

        for cp in extra:
            cp.start()

        @pl.loop(0, n_piece)
        def _(n):
            pltpu.make_async_copy(wz_h.at[layer, :, cols(n)], wz.at[layer, n], w_sem.at[3]).start()

        @pl.loop(0, 2 * n_piece)
        def _(n):
            pltpu.make_async_copy(wo_h.at[layer, :, cols(n)], wo.at[layer, n // n_piece, n % n_piece], w_sem.at[4]).start()

    def bc_copy(layer):
        return pltpu.make_async_copy(wbc_h.at[layer], wbd.at[layer, :, pl.ds(0, 2 * HEAD)], w_sem.at[0])

    def weight_waits(layer):
        whole = lambda ref, sem: pltpu.make_async_copy(ref, ref, w_sem.at[sem])
        return [whole(wbd.at[layer, :, pl.ds(0, 2 * HEAD)], 0), whole(wx.at[layer, pl.ds(0, 2)], 1), whole(wx.at[layer, pl.ds(2, 2)], 2), whole(wz.at[layer], 3), whole(wo.at[layer], 4)]

    first_wait = weight_waits(0)
    for cp in [smalls[0], smalls[-1], hid_copy(0), bc_copy(0)]:
        cp.start()
    start_weights(0, smalls[1:-1])
    for q in range(1, n_subs):
        hid_copy(q).start()

    def remote(src, dst, sem, recv_sem, target):
        return pltpu.make_async_remote_copy(src_ref=src, dst_ref=dst, send_sem=send_sem.at[sem], recv_sem=recv_sem, device_id={"tp": target}, device_id_type=MESH)

    last = layers * n_subs - 1

    def own_slot(s, m):
        return s + m * (s // last)

    def p_copy(s, m):
        return remote(psend.at[s, m], prcv.at[s, m], 0, pr_sem.at[s % 2, m], peer)

    def pstat_copy(s):
        return remote(pstat.at[core, s], pstat.at[core, s], 1, ptr_sem.at[s % 2], peer)

    def q_copy(s, m):
        return remote(qbuf.at[chip, s, m], qbuf.at[chip, s, m], 2, qr_sem.at[own_slot(s, m)], cross)

    def qstat_copy(s):
        return remote(qstat.at[chip, s], qstat.at[chip, s], 3, qtr_sem.at[s], cross)

    def u_copy(s, m):
        spot = ubuf.at[s // n_subs + 1, core, s % n_subs, m]
        return remote(spot, spot, 4, ur_sem.at[own_slot(s, m)], peer)

    def q_arrived(s):
        remote(qbuf.at[chip, s], qbuf.at[chip, s], 2, qr_sem.at[s], cross).wait_recv()

    def u_arrived(s):
        spot = ubuf.at[s // n_subs + 1, core, s % n_subs]
        remote(spot, spot, 4, ur_sem.at[s], peer).wait_recv()

    def all_sent():
        shared = ubuf.at[pl.ds(1, layers), core]
        for sem, ref in enumerate((psend, pstat.at[core], qbuf.at[chip], qstat.at[chip], shared)):
            remote(ref, ref, sem, qtr_sem.at[0], cross).wait_send()

    row64 = iota((SUB, PIECE), 0)
    lane64 = iota((SUB, PIECE), 1) % HEAD
    eye = row64 == lane64
    causal = row64 >= lane64
    low_head = iota((SUB, 128), 1) < HEAD

    def to_row(col):
        return jnp.sum(jnp.where(eye, col, 0.0), axis=0, keepdims=True)

    def to_col(row):
        return jnp.sum(jnp.where(eye[:, :HEAD], row[:, :HEAD], 0.0), axis=1, keepdims=True)

    def scale_of(square_sum):
        return lax.rsqrt(square_sum / inner + EPSILON) * (1.0 / 64.0)

    def inverse_of(square_sum):
        return jnp.where(square_sum < jnp.inf, 64.0 * jnp.sqrt(square_sum / inner + EPSILON), 0.0)

    def head_blocks(part):
        left, right = part[:, :128], part[:, 128:]
        none = jnp.zeros_like(left)
        rows = [jnp.concatenate([jnp.where(low_head, left, 0.0), none], axis=1), jnp.concatenate([jnp.where(low_head, 0.0, left), none], axis=1),
                jnp.concatenate([none, jnp.where(low_head, right, 0.0)], axis=1), jnp.concatenate([none, jnp.where(low_head, 0.0, right)], axis=1)]
        return jnp.concatenate(rows, axis=0).astype(BF16)

    def row_of(ref, layer, lanes=slice(None)):
        row = ref[0:1, lanes]
        for at in range(1, layers):
            row = jnp.where(layer == at, ref[at : at + 1, lanes], row)
        return row.astype(F32)

    def turn_wdt(layer):
        for k in range(0, wdt.shape[2], 128):
            block = wdt[layer, :, k : k + 128].astype(F32)
            turned = jnp.transpose(jnp.concatenate([block] * 3, axis=0)).astype(BF16)
            wbd[layer, k : k + 128, 2 * HEAD : 2 * HEAD + turned.shape[1]] = turned

    def start_layer():
        state[...] = jnp.zeros_like(state)
        x0s[0:8] = jnp.zeros((8, local), F32)
        q0s[0:8] = jnp.zeros((8, q0s.shape[1]), F32)

    def tap_sum(buf, size, lanes, kern, bias):
        total = bias
        for j in range(4):
            total = total + buf[5 + j : 5 + j + size, lanes] * kern[j : j + 1].astype(F32)
        return total

    def norm(layer, q, subs):
        square = [jnp.zeros((SUB, 1), F32) for _ in range(subs)]
        for r in range(subs):
            for side in range(2):
                for m in range(n_piece):
                    val = ubuf[layer, side, q + r, m]
                    square[r] = square[r] + jnp.sum(val * val, axis=1, keepdims=True)
        norm_row = row_of(nw, layer)
        for r in range(subs):
            scale = lax.rsqrt(square[r] / (2 * half) + EPSILON)
            for side in range(2):
                for m in range(n_piece):
                    at = side * half + m * PIECE
                    hbuf[r * SUB : (r + 1) * SUB, at : at + PIECE] = (ubuf[layer, side, q + r, m] * scale * norm_row[:, at : at + PIECE]).astype(BF16)

    def head(layer, q, subs, first, hook):
        size = subs * SUB
        if first:
            first_wait[0].wait()
        both = dot(hbuf[:size], wbd[layer]).astype(BF16).astype(F32)
        q0s[8 : 8 + size, :] = both[:, : 2 * HEAD]
        r_pre = both[:, 2 * HEAD : 2 * HEAD + 3 * (local // HEAD)]
        for n in range(n_piece):
            at = slice(n * PIECE, (n + 1) * PIECE)
            if first and n % 2 == 0:
                first_wait[1 + n // 2].wait()
            x0s[8 : 8 + size, at] = dot(hbuf[:size], wx[layer, n]).astype(BF16).astype(F32)
            if n == 1:
                hook()
        if first:
            for cp in smalls[1:-1]:
                cp.wait()
        bc = jax.nn.silu(tap_sum(q0s, size, slice(None), cbc[layer], row_of(bbc, layer)))
        q0s[0:8] = q0s[size : size + 8]
        triple = lambda ref: jnp.concatenate([row_of(ref, layer)] * 3, axis=1)
        dt_in = r_pre + triple(dtb)
        dt_val = jnp.maximum(dt_in, 0.0) + jnp.log1p(jnp.exp(-jnp.abs(dt_in)))
        a_vals = -dt_val * jnp.exp(triple(al))
        to_t, from_t = iota((size, 3 * size), 0), iota((size, 3 * size), 1) % size
        tri = jnp.where((to_t >= from_t) & (to_t // SUB == from_t // SUB), 1.0, 0.0).astype(BF16)
        a_cum = dot(tri, stack3(a_vals))
        skip = jnp.broadcast_to(triple(ds), (8, a_cum.shape[1]))
        to_spread = jnp.concatenate([dt_val, a_cum, skip], axis=0)
        hi, mid, lo = split3(to_spread)
        lane = iota(to_spread.shape, 1)
        n_heads = local // HEAD
        spread_in = jnp.where(lane < n_heads, hi, jnp.where(lane < 2 * n_heads, mid, lo)).astype(BF16)
        for n in range(n_piece):
            at = slice(n * PIECE, (n + 1) * PIECE)
            group = n * (PIECE // HEAD)
            pick = jnp.where(iota((3 * n_heads, PIECE), 1) // HEAD + group == iota((3 * n_heads, PIECE), 0) % n_heads, 1.0, 0.0).astype(BF16)
            spread[: 2 * size + 8, at] = dot(spread_in, pick)
        swapped = pltpu.roll(bc, HEAD, 1)
        turned = jnp.transpose(bc)
        c_stack, bt_stack, cb = [], [], []
        for r in range(subs):
            rows = slice(r * SUB, (r + 1) * SUB)
            c_stack.append(stack3(swapped[rows, :HEAD]))
            bt_stack.append(stack3(turned[:HEAD, rows]))
            cb.append(exact_dot(c_stack[r], [jnp.concatenate([part] * 4, axis=0).astype(BF16) for part in split3(bc[rows, :HEAD])], dot_nt))
        for n in range(n_piece):
            at = slice(n * PIECE, (n + 1) * PIECE)
            xs[:size, at] = jax.nn.silu(tap_sum(x0s, size, at, cx[layer, :, at], row_of(bx, layer, at)))
            x0s[0:8, at] = x0s[size : size + 8, at]
        if first:
            first_wait[3].wait()
        for n in range(n_piece):
            at = slice(n * PIECE, (n + 1) * PIECE)
            zs[:size, at] = jax.nn.silu(dot(hbuf[:size], wz[layer, n]).astype(BF16).astype(F32))
        for r in range(subs):
            rows = slice(r * SUB, (r + 1) * SUB)
            for n in range(n_piece):
                at = slice(n * PIECE, (n + 1) * PIECE)
                a_e = spread[size + r * SUB : size + (r + 1) * SUB, at]
                decay = jnp.where(causal, jnp.exp(jnp.minimum(a_e - to_row(a_e), 0.0)), 0.0) * cb[r]
                x_dt = xs[rows, at] * spread[rows, at]
                ys[rows, at] = exact_dot(stack3(decay), [head_blocks(part) for part in split3(x_dt)])
        for r in range(subs):
            rows = slice(r * SUB, (r + 1) * SUB)
            for n in range(n_piece):
                at = slice(n * PIECE, (n + 1) * PIECE)
                a_e = spread[size + r * SUB : size + (r + 1) * SUB, at]
                a_last = a_e[SUB - 1 : SUB]
                old = state[:, at]
                carried = exact_dot(c_stack[r], [part.astype(BF16) for part in split3(old)])
                x_act = xs[rows, at]
                ys[rows, at] = ys[rows, at] + carried * jnp.exp(a_e) + spread[2 * size : 2 * size + 1, at] * x_act
                tail_x = x_act * spread[rows, at] * jnp.exp(a_last - a_e)
                state[:, at] = jnp.exp(a_last) * old + exact_dot(bt_stack[r], [part.astype(BF16) for part in split3(tail_x)])

    def tail(layer, q, subs, first):
        size = subs * SUB
        s = layer * n_subs + q
        gate_sq = jnp.zeros((size, 1), F32)
        for n in range(n_piece):
            at = slice(n * PIECE, (n + 1) * PIECE)
            v = ys[:size, at] * zs[:size, at]
            ys[:size, at] = v
            gate_sq = gate_sq + jnp.sum(v * v, axis=1, keepdims=True)
        scale = scale_of(gate_sq)
        gbuf[:size] = (ys[:size] * scale * row_of(gw, layer)).astype(BF16)
        for r in range(subs):
            pstat[core, s + r] = to_row(gate_sq[r * SUB : (r + 1) * SUB])[:, :128]
        if first:
            first_wait[4].wait()
        for m in range(n_piece):
            part = dot(gbuf[:size], wo[layer, 1 - core, m])
            for r in range(subs):
                psend[s + r, m] = part[r * SUB : (r + 1) * SUB]
        if first:
            pl.semaphore_wait(barrier, 2)
        for r in range(subs):
            pstat_copy(s + r).start()
            for m in range(n_piece):
                p_copy(s + r, m).start()
        for m in range(n_piece):
            part = dot(gbuf[:size], wo[layer, core, m])
            for r in range(subs):
                own[m] = part[r * SUB : (r + 1) * SUB]

    def combine(s):
        pstat_copy(s).wait_recv()
        own_sq = to_col(pstat[core, s])
        peer_sq = to_col(pstat[1 - core, s])
        chip_sq = own_sq + peer_sq
        chip_scale = scale_of(chip_sq)
        f_own = chip_scale * inverse_of(own_sq)
        f_peer = chip_scale * inverse_of(peer_sq)
        qstat[chip, s] = to_row(chip_sq)[:, :128]
        qstat_copy(s).start()
        for m in range(n_piece):
            p_copy(s, m).wait_recv()
            qbuf[chip, s, m] = own[m] * f_own + prcv[s, m] * f_peer
            q_copy(s, m).start()

    def update(s, pieces=False):
        layer, c = s // n_subs, s % n_subs
        qstat_copy(s).wait_recv()
        if not pieces:
            q_arrived(s)
        sq0 = to_col(qstat[0, s])
        sq1 = to_col(qstat[1, s])
        norm = lax.rsqrt((sq0 + sq1) / inner + EPSILON)
        f0 = norm * inverse_of(sq0)
        f1 = norm * inverse_of(sq1)
        for m in range(n_piece):
            if pieces:
                q_copy(s, m).wait_recv()
            total = ubuf[layer, core, c, m] + (qbuf[0, s, m] * f0 + qbuf[1, s, m] * f1)
            ubuf[layer + 1, core, c, m] = total.astype(BF16).astype(F32)
            u_copy(s, m).start()

    def emit(s, pieces=False):
        c = s % n_subs
        for side in (core, 1 - core):
            if side is not core and not pieces:
                u_arrived(s)
            for m in range(n_piece):
                if side is not core and pieces:
                    u_copy(s, m).wait_recv()
                cols = pl.ds(pl.multiple_of(side * half + m * PIECE, PIECE), PIECE)
                out_ref[0, pl.ds(pl.multiple_of(c * SUB, SUB), SUB), cols] = ubuf[layers, side, c, m].astype(BF16)

    def load_hidden(c):
        hid_copy(c).wait()
        for side in range(2):
            for m in range(n_piece):
                at = side * half + m * PIECE
                ubuf[0, side, c, m] = hid[c, :, at : at + PIECE].astype(F32)

    steps = layers * n_subs
    lag = n_subs - 1
    steps = layers * n_subs
    lag = n_subs - 1
    start_layer()
    smalls[0].wait()
    load_hidden(0)
    norm(0, 0, 1)
    smalls[-1].wait()
    turn_wdt(0)
    head(0, 0, 1, True, lambda: None)
    tail(0, 0, 1, True)

    bc_copy(1).start()
    start_weights(1)
    combine(0)

    @pl.loop(1, steps)
    def _(t):
        layer, q = t // n_subs, t % n_subs

        @pl.when(t < n_subs)
        def _():
            load_hidden(q)

        @pl.when(t >= n_subs)
        def _():
            u_arrived(t - n_subs)

        for at in range(1, layers):
            @pl.when(t == at * n_subs)
            def _():
                start_layer()
                turn_wdt(at)
                for cp in weight_waits(at):
                    cp.wait()
                if at + 1 < layers:
                    bc_copy(at + 1).start()
                    start_weights(at + 1)

        norm(layer, q, 1)

        @pl.when(t >= lag)
        def _():
            update(t - lag)

        def hook():
            @pl.when(t >= 2)
            def _():
                combine(t - 1)

        head(layer, q, 1, False, hook)
        tail(layer, q, 1, False)

    combine(steps - 1)
    final = steps - n_subs

    @pl.loop(final, steps - 1)
    def _(s):
        @pl.when(s > final)
        def _():
            emit(s - 1)

        @pl.when(s > steps - 1 - lag)
        def _():
            update(s)

    emit(steps - 2)
    update(steps - 1, True)
    emit(steps - 1, True)
    all_sent()


def solution(mesh):
    in_specs = (P('dp'), P(), P(None, None, 'tp'), P(None, None, 'tp'), P(), P(None, None, 'tp'), P(None, None, 'tp'), P(), P(None, 'tp'), P(),
                P(None, 'tp'), P(None, 'tp'), P(None, 'tp'), P(None, 'tp'), P(None, 'tp', None))
    tp_size = mesh.shape['tp']

    def device_forward(hidden, norm_w, w_z, w_x, w_bc, w_dt, conv_x, conv_bc, bias_x, bias_bc, dt_bias, a_log, d_skip, gate_w, w_out):
        layers, width, local = w_x.shape
        n_subs = hidden.shape[1] // SUB
        n_piece = local // PIECE
        steps = layers * n_subs
        bc_width = w_bc.shape[-1]
        w_dt = jnp.swapaxes(w_dt, 1, 2)
        vm = lambda shape, dtype: pltpu.VMEM(shape, dtype)
        same = lambda arr: pltpu.VMEM(arr.shape, arr.dtype)
        scratch = [
            vm((n_subs, SUB, width), BF16), same(norm_w), vm((layers, n_piece, width, PIECE), BF16), vm((layers, n_piece, width, PIECE), BF16),
            vm((layers, width, PIECE), BF16), same(w_dt), same(conv_x), same(conv_bc), same(bias_x), same(bias_bc), same(dt_bias), same(a_log), same(d_skip), same(gate_w),
            vm((layers, 2, n_piece, local, PIECE), BF16),
            vm((layers + 1, 2, n_subs, n_piece, SUB, PIECE), F32),
            vm((steps, n_piece, SUB, PIECE), F32), vm((steps, n_piece, SUB, PIECE), F32), vm((2, steps, n_piece, SUB, PIECE), F32),
            vm((2, steps, 1, 128), F32), vm((2, steps, 1, 128), F32),
            vm((n_piece, SUB, PIECE), F32), vm((MAX_ROWS, width), BF16), vm((MAX_ROWS + 8, local), F32), vm((MAX_ROWS + 8, bc_width), F32),
            vm((MAX_ROWS, local), F32), vm((MAX_ROWS, local), F32), vm((MAX_ROWS, local), F32), vm((2 * MAX_ROWS + 8, local), F32), vm((HEAD, local), F32), vm((MAX_ROWS, local), BF16),
            pltpu.SemaphoreType.DMA((10,)), pltpu.SemaphoreType.DMA((n_subs,)), pltpu.SemaphoreType.DMA((5,)), pltpu.SemaphoreType.DMA((5,)),
            pltpu.SemaphoreType.DMA((2, n_piece)), pltpu.SemaphoreType.DMA((steps - 1 + n_piece,)), pltpu.SemaphoreType.DMA((steps - 1 + n_piece,)),
            pltpu.SemaphoreType.DMA((2,)), pltpu.SemaphoreType.DMA((steps,)),
        ]
        return pl.pallas_call(
            functools.partial(kernel, float(local * tp_size)),
            out_shape=jax.ShapeDtypeStruct(hidden.shape, hidden.dtype),
            in_specs=[pl.BlockSpec(memory_space=pltpu.HBM)] * 15,
            out_specs=pl.BlockSpec(memory_space=pltpu.VMEM),
            scratch_shapes=scratch,
            compiler_params=pltpu.CompilerParams(collective_id=0, has_side_effects=True, vmem_limit_bytes=52 * 1024 * 1024),
        )(*[pltpu.with_memory_space_constraint(arr, pltpu.HBM) for arr in (hidden, norm_w, w_z, w_x, w_bc, w_dt, conv_x, conv_bc, bias_x, bias_bc, dt_bias, a_log, d_skip, gate_w, w_out)])

    return jax.shard_map(device_forward, mesh=mesh, in_specs=in_specs, out_specs=P('dp'), check_vma=False)
```

```python
import functools

import jax
import jax.numpy as jnp
from jax import lax
from jax.experimental import pallas as pl
from jax.experimental.pallas import tpu as pltpu
from jax.sharding import PartitionSpec as P

EPSILON = 1e-5
MESH = pl.DeviceIdType.MESH
SUB = 64
MAX_ROWS = 64
ORDER_FIRST = "x2 i0 x3 i1 c2 a0 c3 a1 i2 a2 i3 a3 wait z0 z1 z2 z3"
ORDER_LATER = "c0 z0 c1 i0 c2 z1 i1 a0 c3 z2 i2 a1 z3 i3 a2 a3"
PIECE = 256
HEAD = 64
F32 = jnp.float32
BF16 = jnp.bfloat16


def split3(val):
    hi = val.astype(BF16).astype(F32)
    rest = val - hi
    mid = rest.astype(BF16).astype(F32)
    return hi, mid, rest - mid


def stack3(val):
    return jnp.concatenate(split3(val), axis=0).astype(BF16)


def dot(a, b):
    return lax.dot_general(a, b, (((1,), (0,)), ((), ())), preferred_element_type=F32)


def dot_nt(a, b):
    return lax.dot_general(a, b, (((1,), (1,)), ((), ())), preferred_element_type=F32)


def exact_dot(a_stack, b_parts, product=dot):
    rows = a_stack.shape[0] // 3
    b_hi, b_mid, b_lo = b_parts
    r1 = product(a_stack, b_hi)
    r2 = product(a_stack[: 2 * rows], b_mid)
    r3 = product(a_stack[:rows], b_lo)
    small = r1[2 * rows :] + r2[rows:] + r3
    return r1[:rows] + (r1[rows : 2 * rows] + r2[:rows] + small)


def iota(shape, dim):
    return lax.broadcasted_iota(jnp.int32, shape, dim)


def kernel(inner, hid_h, nw_h, wz_h, wx_h, wbc_h, wdt_h, cx_h, cbc_h, bx_h, bbc_h, dtb_h, al_h, ds_h, gw_h, wo_h,
           out_ref, hid, nw, wz, wx, wbd, wdt, cx, cbc, bx, bbc, dtb, al, ds, gw, wo,
           ubuf, psend, prcv, qbuf, pstat, qstat, own, hbuf, x0s, q0s, xs, ys, zs, dstack, spread, state, gbuf,
           small_sem, hid_sem, w_sem, send_sem, pr_sem, qr_sem, ur_sem, ptr_sem, qtr_sem):
    me = lax.axis_index("tp")
    core = me % 2
    chip = me // 2
    peer = me + 1 - 2 * core
    cross = (me + 2) % 4
    n_subs = hid_h.shape[1] // SUB
    n_piece = wx_h.shape[2] // PIECE
    layers = nw_h.shape[0]
    local = wx_h.shape[2]
    half = wo_h.shape[2] // 2

    barrier = pltpu.get_barrier_semaphore()
    for other in (peer, cross):
        pl.semaphore_signal(barrier, inc=1, device_id={"tp": other}, device_id_type=MESH)

    smalls = [pltpu.make_async_copy(src, dst, small_sem.at[i]) for i, (src, dst) in enumerate(
        [(nw_h, nw), (cx_h, cx), (cbc_h, cbc), (bx_h, bx), (bbc_h, bbc), (dtb_h, dtb), (al_h, al), (ds_h, ds), (gw_h, gw), (wdt_h, wdt)])]

    def hid_copy(c):
        return pltpu.make_async_copy(hid_h.at[0, pl.ds(c * SUB, SUB)], hid.at[c], hid_sem.at[c])

    def start_weights(layer):
        cols = lambda n: pl.ds(pl.multiple_of(n * PIECE, PIECE), PIECE)

        @pl.loop(0, n_piece)
        def _(n):
            pltpu.make_async_copy(wx_h.at[layer, :, cols(n)], wx.at[layer, n], w_sem.at[1 + n // 2]).start()

        @pl.loop(0, n_piece)
        def _(n):
            pltpu.make_async_copy(wz_h.at[layer, :, cols(n)], wz.at[layer, n], w_sem.at[3]).start()

        @pl.loop(0, 2 * n_piece)
        def _(n):
            side = (n // n_piece + 1 - core) % 2
            pltpu.make_async_copy(wo_h.at[layer, :, cols(side * n_piece + n % n_piece)], wo.at[layer, side, n % n_piece], w_sem.at[4 + n // n_piece]).start()

    def bc_copy(layer):
        return pltpu.make_async_copy(wbc_h.at[layer], wbd.at[layer, :, pl.ds(0, 2 * HEAD)], w_sem.at[0])

    def weight_waits(layer):
        whole = lambda ref, sem: pltpu.make_async_copy(ref, ref, w_sem.at[sem])
        return [whole(wbd.at[layer, :, pl.ds(0, 2 * HEAD)], 0), whole(wx.at[layer, pl.ds(0, 2)], 1), whole(wx.at[layer, pl.ds(2, 2)], 2), whole(wz.at[layer], 3), whole(wo.at[layer, 1 - core], 4), whole(wo.at[layer, core], 5)]

    first_wait = weight_waits(0)
    for cp in [smalls[0], smalls[-1], hid_copy(0), bc_copy(0)] + smalls[1:-1]:
        cp.start()
    start_weights(0)
    for q in range(1, n_subs):
        hid_copy(q).start()

    def remote(src, dst, sem, recv_sem, target):
        return pltpu.make_async_remote_copy(src_ref=src, dst_ref=dst, send_sem=send_sem.at[sem], recv_sem=recv_sem, device_id={"tp": target}, device_id_type=MESH)

    last = layers * n_subs - 1

    def own_slot(s, m):
        return s + m * (s // last)

    def p_copy(s, m):
        return remote(psend.at[s, m], prcv.at[s, m], 0, pr_sem.at[s % 2, m], peer)

    def pstat_copy(s):
        return remote(pstat.at[core, s], pstat.at[core, s], 1, ptr_sem.at[s % 2], peer)

    def q_copy(s, m):
        return remote(qbuf.at[chip, s, m], qbuf.at[chip, s, m], 2, qr_sem.at[own_slot(s, m)], cross)

    def qstat_copy(s):
        return remote(qstat.at[chip, s], qstat.at[chip, s], 3, qtr_sem.at[s], cross)

    def u_copy(s, m):
        spot = ubuf.at[s // n_subs + 1, core, s % n_subs, m]
        return remote(spot, spot, 4, ur_sem.at[own_slot(s, m)], peer)

    def q_arrived(s):
        remote(qbuf.at[chip, s], qbuf.at[chip, s], 2, qr_sem.at[s], cross).wait_recv()

    def u_arrived(s):
        spot = ubuf.at[s // n_subs + 1, core, s % n_subs]
        remote(spot, spot, 4, ur_sem.at[s], peer).wait_recv()

    def all_sent():
        shared = ubuf.at[pl.ds(1, layers), core]
        for sem, ref in enumerate((psend, pstat.at[core], qbuf.at[chip], qstat.at[chip], shared)):
            remote(ref, ref, sem, qtr_sem.at[0], cross).wait_send()

    row64 = iota((SUB, PIECE), 0)
    lane64 = iota((SUB, PIECE), 1) % HEAD
    eye = row64 == lane64
    causal = row64 >= lane64
    low_head = iota((SUB, 128), 1) < HEAD

    def to_row(col):
        return jnp.sum(jnp.where(eye, col, 0.0), axis=0, keepdims=True)

    def to_col(row):
        return jnp.sum(jnp.where(eye[:, :HEAD], row[:, :HEAD], 0.0), axis=1, keepdims=True)

    def scale_of(square_sum):
        return lax.rsqrt(square_sum / inner + EPSILON) * (1.0 / 64.0)

    def inverse_of(square_sum):
        return jnp.where(square_sum < jnp.inf, 64.0 * jnp.sqrt(square_sum / inner + EPSILON), 0.0)

    def head_blocks(part):
        left, right = part[:, :128], part[:, 128:]
        none = jnp.zeros_like(left)
        rows = [jnp.concatenate([jnp.where(low_head, left, 0.0), none], axis=1), jnp.concatenate([jnp.where(low_head, 0.0, left), none], axis=1),
                jnp.concatenate([none, jnp.where(low_head, right, 0.0)], axis=1), jnp.concatenate([none, jnp.where(low_head, 0.0, right)], axis=1)]
        return jnp.concatenate(rows, axis=0).astype(BF16)

    def row_of(ref, layer, lanes=slice(None)):
        row = ref[0:1, lanes]
        for at in range(1, layers):
            row = jnp.where(layer == at, ref[at : at + 1, lanes], row)
        return row.astype(F32)

    def turn_wdt(layer):
        for k in range(0, wdt.shape[2], 128):
            block = wdt[layer, :, k : k + 128].astype(F32)
            turned = jnp.transpose(jnp.concatenate([block] * 3, axis=0)).astype(BF16)
            wbd[layer, k : k + 128, 2 * HEAD : 2 * HEAD + turned.shape[1]] = turned

    def start_layer():
        state[...] = jnp.zeros_like(state)
        x0s[0:8] = jnp.zeros((8, local), F32)
        q0s[0:8] = jnp.zeros((8, q0s.shape[1]), F32)

    def tap_sum(buf, size, lanes, kern, bias):
        total = bias
        for j in range(4):
            total = total + buf[5 + j : 5 + j + size, lanes] * kern[j : j + 1].astype(F32)
        return total

    def norm(layer, q, subs):
        square = [jnp.zeros((SUB, 1), F32) for _ in range(subs)]
        for r in range(subs):
            for side in range(2):
                for m in range(n_piece):
                    val = ubuf[layer, side, q + r, m]
                    square[r] = square[r] + jnp.sum(val * val, axis=1, keepdims=True)
        norm_row = row_of(nw, layer)
        for r in range(subs):
            scale = lax.rsqrt(square[r] / (2 * half) + EPSILON)
            for side in range(2):
                for m in range(n_piece):
                    at = side * half + m * PIECE
                    hbuf[r * SUB : (r + 1) * SUB, at : at + PIECE] = (ubuf[layer, side, q + r, m] * scale * norm_row[:, at : at + PIECE]).astype(BF16)

    def x_product(layer, size, n):
        x0s[8 : 8 + size, n * PIECE : (n + 1) * PIECE] = dot(hbuf[:size], wx[layer, n]).astype(BF16).astype(F32)

    def z_product(layer, size, n):
        zs[:size, n * PIECE : (n + 1) * PIECE] = jax.nn.silu(dot(hbuf[:size], wz[layer, n]).astype(BF16).astype(F32))

    def head(layer, q, subs, first, hook):
        size = subs * SUB
        if first:
            first_wait[0].wait()
        both = dot(hbuf[:size], wbd[layer]).astype(BF16).astype(F32)
        q0s[8 : 8 + size, :] = both[:, : 2 * HEAD]
        r_pre = both[:, 2 * HEAD : 2 * HEAD + 3 * (local // HEAD)]
        if first:
            for cp in smalls[1:-1]:
                cp.wait()
        if not first:
            x_product(layer, size, 0)
            x_product(layer, size, 1)
            hook()
            x_product(layer, size, 2)
            x_product(layer, size, 3)
        bc = jax.nn.silu(tap_sum(q0s, size, slice(None), cbc[layer], row_of(bbc, layer)))
        q0s[0:8] = q0s[size : size + 8]
        triple = lambda ref: jnp.concatenate([row_of(ref, layer)] * 3, axis=1)
        dt_in = r_pre + triple(dtb)
        dt_val = jnp.maximum(dt_in, 0.0) + jnp.log1p(jnp.exp(-jnp.abs(dt_in)))
        a_vals = -dt_val * jnp.exp(triple(al))
        to_t, from_t = iota((size, 3 * size), 0), iota((size, 3 * size), 1) % size
        tri = jnp.where((to_t >= from_t) & (to_t // SUB == from_t // SUB), 1.0, 0.0).astype(BF16)
        a_cum = dot(tri, stack3(a_vals))
        skip = jnp.broadcast_to(triple(ds), (8, a_cum.shape[1]))
        to_spread = jnp.concatenate([dt_val, a_cum, skip], axis=0)
        hi, mid, lo = split3(to_spread)
        lane = iota(to_spread.shape, 1)
        n_heads = local // HEAD
        spread_in = jnp.where(lane < n_heads, hi, jnp.where(lane < 2 * n_heads, mid, lo)).astype(BF16)
        for n in range(n_piece):
            at = slice(n * PIECE, (n + 1) * PIECE)
            group = n * (PIECE // HEAD)
            pick = jnp.where(iota((3 * n_heads, PIECE), 1) // HEAD + group == iota((3 * n_heads, PIECE), 0) % n_heads, 1.0, 0.0).astype(BF16)
            spread[: 2 * size + 8, at] = dot(spread_in, pick)
        swapped = pltpu.roll(bc, HEAD, 1)
        turned = jnp.transpose(bc)
        c_stack, bt_stack, cb = [], [], []
        for r in range(subs):
            rows = slice(r * SUB, (r + 1) * SUB)
            c_stack.append(stack3(swapped[rows, :HEAD]))
            bt_stack.append(stack3(turned[:HEAD, rows]))
            cb.append(exact_dot(c_stack[r], [jnp.concatenate([part] * 4, axis=0).astype(BF16) for part in split3(bc[rows, :HEAD])], dot_nt))
        for r in range(subs):
            rows = slice(3 * r * SUB, 3 * (r + 1) * SUB)
            for n in range(n_piece):
                at = slice(n * PIECE, (n + 1) * PIECE)
                a_e = spread[size + r * SUB : size + (r + 1) * SUB, at]
                dstack[rows, at] = stack3(jnp.where(causal, jnp.exp(jnp.minimum(a_e - to_row(a_e), 0.0)), 0.0) * cb[r])

        def conv(n):
            at = slice(n * PIECE, (n + 1) * PIECE)
            xs[:size, at] = jax.nn.silu(tap_sum(x0s, size, at, cx[layer, :, at], row_of(bx, layer, at)))
            x0s[0:8, at] = x0s[size : size + 8, at]

        def inside(n):
            at = slice(n * PIECE, (n + 1) * PIECE)
            for r in range(subs):
                rows = slice(r * SUB, (r + 1) * SUB)
                x_dt = xs[rows, at] * spread[rows, at]
                ys[rows, at] = exact_dot(dstack[3 * r * SUB : 3 * (r + 1) * SUB, at], [head_blocks(part) for part in split3(x_dt)])

        def across(n):
            at = slice(n * PIECE, (n + 1) * PIECE)
            for r in range(subs):
                rows = slice(r * SUB, (r + 1) * SUB)
                a_e = spread[size + r * SUB : size + (r + 1) * SUB, at]
                a_last = a_e[SUB - 1 : SUB]
                old = state[:, at]
                carried = exact_dot(c_stack[r], [part.astype(BF16) for part in split3(old)])
                x_act = xs[rows, at]
                ys[rows, at] = ys[rows, at] + carried * jnp.exp(a_e) + spread[2 * size : 2 * size + 1, at] * x_act
                tail_x = x_act * spread[rows, at] * jnp.exp(a_last - a_e)
                state[:, at] = jnp.exp(a_last) * old + exact_dot(bt_stack[r], [part.astype(BF16) for part in split3(tail_x)])

        if first:
            first_wait[1].wait()
            x_product(layer, size, 0)
            x_product(layer, size, 1)
            conv(0)
            conv(1)
            first_wait[2].wait()
        plan = ORDER_FIRST if first else ORDER_LATER
        stages = {"x": lambda n: x_product(layer, size, n), "c": conv, "i": inside, "a": across, "z": lambda n: z_product(layer, size, n)}
        for step in plan.split():
            if step == "wait":
                first_wait[3].wait()
            else:
                stages[step[0]](int(step[1]))

    def tail(layer, q, subs, first):
        size = subs * SUB
        s = layer * n_subs + q
        gate_sq = jnp.zeros((size, 1), F32)
        for n in range(n_piece):
            at = slice(n * PIECE, (n + 1) * PIECE)
            v = ys[:size, at] * zs[:size, at]
            ys[:size, at] = v
            gate_sq = gate_sq + jnp.sum(v * v, axis=1, keepdims=True)
        scale = scale_of(gate_sq)
        gbuf[:size] = (ys[:size] * scale * row_of(gw, layer)).astype(BF16)
        for r in range(subs):
            pstat[core, s + r] = to_row(gate_sq[r * SUB : (r + 1) * SUB])[:, :128]
        if first:
            first_wait[4].wait()
        for m in range(n_piece):
            part = dot(gbuf[:size], wo[layer, 1 - core, m])
            for r in range(subs):
                psend[s + r, m] = part[r * SUB : (r + 1) * SUB]
        if first:
            pl.semaphore_wait(barrier, 2)
        for r in range(subs):
            pstat_copy(s + r).start()
            for m in range(n_piece):
                p_copy(s + r, m).start()
        if first:
            first_wait[5].wait()
        for m in range(n_piece):
            part = dot(gbuf[:size], wo[layer, core, m])
            for r in range(subs):
                own[m] = part[r * SUB : (r + 1) * SUB]

    def combine(s):
        pstat_copy(s).wait_recv()
        own_sq = to_col(pstat[core, s])
        peer_sq = to_col(pstat[1 - core, s])
        chip_sq = own_sq + peer_sq
        chip_scale = scale_of(chip_sq)
        f_own = chip_scale * inverse_of(own_sq)
        f_peer = chip_scale * inverse_of(peer_sq)
        qstat[chip, s] = to_row(chip_sq)[:, :128]
        qstat_copy(s).start()
        for m in range(n_piece):
            p_copy(s, m).wait_recv()
            qbuf[chip, s, m] = own[m] * f_own + prcv[s, m] * f_peer
            q_copy(s, m).start()

    def update(s, pieces=False):
        layer, c = s // n_subs, s % n_subs
        qstat_copy(s).wait_recv()
        if not pieces:
            q_arrived(s)
        sq0 = to_col(qstat[0, s])
        sq1 = to_col(qstat[1, s])
        norm = lax.rsqrt((sq0 + sq1) / inner + EPSILON)
        f0 = norm * inverse_of(sq0)
        f1 = norm * inverse_of(sq1)
        for m in range(n_piece):
            if pieces:
                q_copy(s, m).wait_recv()
            total = ubuf[layer, core, c, m] + (qbuf[0, s, m] * f0 + qbuf[1, s, m] * f1)
            ubuf[layer + 1, core, c, m] = total.astype(BF16).astype(F32)
            u_copy(s, m).start()

    def emit(s, pieces=False):
        c = s % n_subs
        for side in (core, 1 - core):
            if side is not core and not pieces:
                u_arrived(s)
            for m in range(n_piece):
                if side is not core and pieces:
                    u_copy(s, m).wait_recv()
                cols = pl.ds(pl.multiple_of(side * half + m * PIECE, PIECE), PIECE)
                out_ref[0, pl.ds(pl.multiple_of(c * SUB, SUB), SUB), cols] = ubuf[layers, side, c, m].astype(BF16)

    def load_hidden(c):
        hid_copy(c).wait()
        for side in range(2):
            for m in range(n_piece):
                at = side * half + m * PIECE
                ubuf[0, side, c, m] = hid[c, :, at : at + PIECE].astype(F32)

    steps = layers * n_subs
    lag = n_subs - 1
    steps = layers * n_subs
    lag = n_subs - 1
    start_layer()
    smalls[0].wait()
    smalls[-1].wait()
    turn_wdt(0)
    load_hidden(0)
    norm(0, 0, 1)
    head(0, 0, 1, True, lambda: None)
    tail(0, 0, 1, True)

    bc_copy(1).start()
    start_weights(1)
    combine(0)

    @pl.loop(1, steps)
    def _(t):
        layer, q = t // n_subs, t % n_subs

        @pl.when(t < n_subs)
        def _():
            load_hidden(q)

        @pl.when(t >= n_subs)
        def _():
            u_arrived(t - n_subs)

        for at in range(1, layers):
            @pl.when(t == at * n_subs)
            def _():
                start_layer()
                turn_wdt(at)
                for cp in weight_waits(at):
                    cp.wait()
                if at + 1 < layers:
                    bc_copy(at + 1).start()
                    start_weights(at + 1)

        norm(layer, q, 1)

        @pl.when(t == 2)
        def _():
            combine(t - 1)

        @pl.when(t >= lag)
        def _():
            update(t - lag)

        def hook():
            @pl.when(t > 2)
            def _():
                combine(t - 1)

        head(layer, q, 1, False, hook)
        tail(layer, q, 1, False)

    combine(steps - 1)
    final = steps - n_subs

    @pl.loop(final, steps - 1)
    def _(s):
        @pl.when(s > final)
        def _():
            emit(s - 1)

        @pl.when(s > steps - 1 - lag)
        def _():
            update(s)

    emit(steps - 2)
    update(steps - 1, True)
    emit(steps - 1, True)
    all_sent()


def solution(mesh):
    in_specs = (P('dp'), P(), P(None, None, 'tp'), P(None, None, 'tp'), P(), P(None, None, 'tp'), P(None, None, 'tp'), P(), P(None, 'tp'), P(),
                P(None, 'tp'), P(None, 'tp'), P(None, 'tp'), P(None, 'tp'), P(None, 'tp', None))
    tp_size = mesh.shape['tp']

    def device_forward(hidden, norm_w, w_z, w_x, w_bc, w_dt, conv_x, conv_bc, bias_x, bias_bc, dt_bias, a_log, d_skip, gate_w, w_out):
        layers, width, local = w_x.shape
        n_subs = hidden.shape[1] // SUB
        n_piece = local // PIECE
        steps = layers * n_subs
        bc_width = w_bc.shape[-1]
        w_dt = jnp.swapaxes(w_dt, 1, 2)
        vm = lambda shape, dtype: pltpu.VMEM(shape, dtype)
        same = lambda arr: pltpu.VMEM(arr.shape, arr.dtype)
        scratch = [
            vm((n_subs, SUB, width), BF16), same(norm_w), vm((layers, n_piece, width, PIECE), BF16), vm((layers, n_piece, width, PIECE), BF16),
            vm((layers, width, PIECE), BF16), same(w_dt), same(conv_x), same(conv_bc), same(bias_x), same(bias_bc), same(dt_bias), same(a_log), same(d_skip), same(gate_w),
            vm((layers, 2, n_piece, local, PIECE), BF16),
            vm((layers + 1, 2, n_subs, n_piece, SUB, PIECE), F32),
            vm((steps, n_piece, SUB, PIECE), F32), vm((steps, n_piece, SUB, PIECE), F32), vm((2, steps, n_piece, SUB, PIECE), F32),
            vm((2, steps, 1, 128), F32), vm((2, steps, 1, 128), F32),
            vm((n_piece, SUB, PIECE), F32), vm((MAX_ROWS, width), BF16), vm((MAX_ROWS + 8, local), F32), vm((MAX_ROWS + 8, bc_width), F32),
            vm((MAX_ROWS, local), F32), vm((MAX_ROWS, local), F32), vm((MAX_ROWS, local), F32), vm((3 * MAX_ROWS, local), BF16), vm((2 * MAX_ROWS + 8, local), F32), vm((HEAD, local), F32), vm((MAX_ROWS, local), BF16),
            pltpu.SemaphoreType.DMA((10,)), pltpu.SemaphoreType.DMA((n_subs,)), pltpu.SemaphoreType.DMA((6,)), pltpu.SemaphoreType.DMA((5,)),
            pltpu.SemaphoreType.DMA((2, n_piece)), pltpu.SemaphoreType.DMA((steps - 1 + n_piece,)), pltpu.SemaphoreType.DMA((steps - 1 + n_piece,)),
            pltpu.SemaphoreType.DMA((2,)), pltpu.SemaphoreType.DMA((steps,)),
        ]
        return pl.pallas_call(
            functools.partial(kernel, float(local * tp_size)),
            out_shape=jax.ShapeDtypeStruct(hidden.shape, hidden.dtype),
            in_specs=[pl.BlockSpec(memory_space=pltpu.HBM)] * 15,
            out_specs=pl.BlockSpec(memory_space=pltpu.VMEM),
            scratch_shapes=scratch,
            compiler_params=pltpu.CompilerParams(collective_id=0, has_side_effects=True, vmem_limit_bytes=52 * 1024 * 1024),
        )(*[pltpu.with_memory_space_constraint(arr, pltpu.HBM) for arr in (hidden, norm_w, w_z, w_x, w_bc, w_dt, conv_x, conv_bc, bias_x, bias_bc, dt_bias, a_log, d_skip, gate_w, w_out)])

    return jax.shard_map(device_forward, mesh=mesh, in_specs=in_specs, out_specs=P('dp'), check_vma=False)
```

```python
import functools

import jax
import jax.numpy as jnp
from jax import lax
from jax.experimental import pallas as pl
from jax.experimental.pallas import tpu as pltpu
from jax.sharding import PartitionSpec as P

EPSILON = 1e-5
MESH = pl.DeviceIdType.MESH
SUB = 64
MAX_ROWS = 64
ORDER_FIRST = ("x2", "i0", "x3", "i1", "c2", "a0", "c3", "a1", "i2", "a2", "i3", "a3", "wait", "z0", "z1", "z2", "z3")
ORDER_LATER = ("c0", "z0", "c1", "i0", "c2", "z1", "i1", "a0", "c3", "z2", "i2", "a1", "z3", "i3", "a2", "a3")
PIECE = 256
HEAD = 64
F32 = jnp.float32
BF16 = jnp.bfloat16


def split3(val):
    hi = val.astype(BF16).astype(F32)
    rest = val - hi
    mid = rest.astype(BF16).astype(F32)
    return hi, mid, rest - mid


def stack3(val):
    return jnp.concatenate(split3(val), axis=0).astype(BF16)


def dot(a, b):
    return lax.dot_general(a, b, (((1,), (0,)), ((), ())), preferred_element_type=F32)


def dot_nt(a, b):
    return lax.dot_general(a, b, (((1,), (1,)), ((), ())), preferred_element_type=F32)


def exact_dot(a_stack, b_parts, product=dot):
    rows = a_stack.shape[0] // 3
    b_hi, b_mid, b_lo = b_parts
    r1 = product(a_stack, b_hi)
    r2 = product(a_stack[: 2 * rows], b_mid)
    r3 = product(a_stack[:rows], b_lo)
    small = r1[2 * rows :] + r2[rows:] + r3
    return r1[:rows] + (r1[rows : 2 * rows] + r2[:rows] + small)


def iota(shape, dim):
    return lax.broadcasted_iota(jnp.int32, shape, dim)


def kernel(inner, hid_h, nw_h, wz_h, wx_h, wbc_h, wdt_h, cx_h, cbc_h, bx_h, bbc_h, dtb_h, al_h, ds_h, gw_h, wo_h,
           out_ref, hid, nw, wz, wx, wbd, wdt, cx, cbc, bx, bbc, dtb, al, ds, gw, wo,
           ubuf, psend, prcv, qbuf, pstat, qstat, own, hbuf, x0s, q0s, xs, ys, zs, dstack, spread, state, gbuf,
           small_sem, hid_sem, w_sem, send_sem, pr_sem, qr_sem, ur_sem, ptr_sem, qtr_sem):
    me = lax.axis_index("tp")
    core = me % 2
    chip = me // 2
    peer = me + 1 - 2 * core
    cross = (me + 2) % 4
    n_subs = hid_h.shape[1] // SUB
    n_piece = wx_h.shape[2] // PIECE
    layers = nw_h.shape[0]
    local = wx_h.shape[2]
    half = wo_h.shape[2] // 2

    barrier = pltpu.get_barrier_semaphore()
    for other in (peer, cross):
        pl.semaphore_signal(barrier, inc=1, device_id={"tp": other}, device_id_type=MESH)

    smalls = [pltpu.make_async_copy(src, dst, small_sem.at[i]) for i, (src, dst) in enumerate(
        [(nw_h, nw), (cx_h, cx), (cbc_h, cbc), (bx_h, bx), (bbc_h, bbc), (dtb_h, dtb), (al_h, al), (ds_h, ds), (gw_h, gw), (wdt_h, wdt)])]

    def hid_copy(c):
        return pltpu.make_async_copy(hid_h.at[0, pl.ds(c * SUB, SUB)], hid.at[c], hid_sem.at[c])

    def start_weights(layer):
        cols = lambda n: pl.ds(pl.multiple_of(n * PIECE, PIECE), PIECE)

        @pl.loop(0, n_piece)
        def _(n):
            pltpu.make_async_copy(wx_h.at[layer, :, cols(n)], wx.at[layer, n], w_sem.at[1 + n // 2]).start()

        @pl.loop(0, n_piece)
        def _(n):
            pltpu.make_async_copy(wz_h.at[layer, :, cols(n)], wz.at[layer, n], w_sem.at[3]).start()

        @pl.loop(0, 2 * n_piece)
        def _(n):
            side = (n // n_piece + 1 - core) % 2
            pltpu.make_async_copy(wo_h.at[layer, :, cols(side * n_piece + n % n_piece)], wo.at[layer, side, n % n_piece], w_sem.at[4 + n // n_piece]).start()

    def bc_copy(layer):
        return pltpu.make_async_copy(wbc_h.at[layer], wbd.at[layer, :, pl.ds(0, 2 * HEAD)], w_sem.at[0])

    def weight_waits(layer):
        whole = lambda ref, sem: pltpu.make_async_copy(ref, ref, w_sem.at[sem])
        return [whole(wbd.at[layer, :, pl.ds(0, 2 * HEAD)], 0), whole(wx.at[layer, pl.ds(0, 2)], 1), whole(wx.at[layer, pl.ds(2, 2)], 2), whole(wz.at[layer], 3), whole(wo.at[layer, 1 - core], 4), whole(wo.at[layer, core], 5)]

    first_wait = weight_waits(0)
    for cp in [smalls[0], smalls[-1], hid_copy(0), bc_copy(0)] + smalls[1:-1]:
        cp.start()
    start_weights(0)
    for q in range(1, n_subs):
        hid_copy(q).start()

    def remote(src, dst, sem, recv_sem, target):
        return pltpu.make_async_remote_copy(src_ref=src, dst_ref=dst, send_sem=send_sem.at[sem], recv_sem=recv_sem, device_id={"tp": target}, device_id_type=MESH)

    last = layers * n_subs - 1

    def own_slot(s, m):
        return s + m * (s // last)

    def p_copy(s, m):
        return remote(psend.at[s, m], prcv.at[s, m], 0, pr_sem.at[s % 2, m], peer)

    def pstat_copy(s):
        return remote(pstat.at[core, s], pstat.at[core, s], 1, ptr_sem.at[s % 2], peer)

    def q_copy(s, m):
        return remote(qbuf.at[chip, s, m], qbuf.at[chip, s, m], 2, qr_sem.at[own_slot(s, m)], cross)

    def qstat_copy(s):
        return remote(qstat.at[chip, s], qstat.at[chip, s], 3, qtr_sem.at[s], cross)

    def u_copy(s, m):
        spot = ubuf.at[s // n_subs + 1, core, s % n_subs, m]
        return remote(spot, spot, 4, ur_sem.at[own_slot(s, m)], peer)

    def q_arrived(s):
        remote(qbuf.at[chip, s], qbuf.at[chip, s], 2, qr_sem.at[s], cross).wait_recv()

    def u_arrived(s):
        spot = ubuf.at[s // n_subs + 1, core, s % n_subs]
        remote(spot, spot, 4, ur_sem.at[s], peer).wait_recv()

    def all_sent():
        shared = ubuf.at[pl.ds(1, layers), core]
        for sem, ref in enumerate((psend, pstat.at[core], qbuf.at[chip], qstat.at[chip], shared)):
            remote(ref, ref, sem, qtr_sem.at[0], cross).wait_send()

    row64 = iota((SUB, PIECE), 0)
    lane64 = iota((SUB, PIECE), 1) % HEAD
    eye = row64 == lane64
    causal = row64 >= lane64
    low_head = iota((SUB, 128), 1) < HEAD

    def to_row(col):
        return jnp.sum(jnp.where(eye, col, 0.0), axis=0, keepdims=True)

    def to_col(row):
        return jnp.sum(jnp.where(eye[:, :HEAD], row[:, :HEAD], 0.0), axis=1, keepdims=True)

    def scale_of(square_sum):
        return lax.rsqrt(square_sum / inner + EPSILON) * (1.0 / 64.0)

    def inverse_of(square_sum):
        return jnp.where(square_sum < jnp.inf, 64.0 * jnp.sqrt(square_sum / inner + EPSILON), 0.0)

    def head_blocks(part):
        left, right = part[:, :128], part[:, 128:]
        none = jnp.zeros_like(left)
        rows = [jnp.concatenate([jnp.where(low_head, left, 0.0), none], axis=1), jnp.concatenate([jnp.where(low_head, 0.0, left), none], axis=1),
                jnp.concatenate([none, jnp.where(low_head, right, 0.0)], axis=1), jnp.concatenate([none, jnp.where(low_head, 0.0, right)], axis=1)]
        return jnp.concatenate(rows, axis=0).astype(BF16)

    def row_of(ref, layer, lanes=slice(None)):
        row = ref[0:1, lanes]
        for at in range(1, layers):
            row = jnp.where(layer == at, ref[at : at + 1, lanes], row)
        return row.astype(F32)

    def turn_wdt(layer):
        for k in range(0, wdt.shape[2], 128):
            block = wdt[layer, :, k : k + 128].astype(F32)
            turned = jnp.transpose(jnp.concatenate([block] * 3, axis=0)).astype(BF16)
            wbd[layer, k : k + 128, 2 * HEAD : 2 * HEAD + turned.shape[1]] = turned

    def start_layer():
        state[...] = jnp.zeros_like(state)
        x0s[0:8] = jnp.zeros((8, local), F32)
        q0s[0:8] = jnp.zeros((8, q0s.shape[1]), F32)

    def tap_sum(buf, size, lanes, kern, bias):
        total = bias
        for j in range(4):
            total = total + buf[5 + j : 5 + j + size, lanes] * kern[j : j + 1].astype(F32)
        return total

    def norm(layer, q, subs):
        square = [jnp.zeros((SUB, 1), F32) for _ in range(subs)]
        for r in range(subs):
            for side in range(2):
                for m in range(n_piece):
                    val = ubuf[layer, side, q + r, m]
                    square[r] = square[r] + jnp.sum(val * val, axis=1, keepdims=True)
        norm_row = row_of(nw, layer)
        for r in range(subs):
            scale = lax.rsqrt(square[r] / (2 * half) + EPSILON)
            for side in range(2):
                for m in range(n_piece):
                    at = side * half + m * PIECE
                    hbuf[r * SUB : (r + 1) * SUB, at : at + PIECE] = (ubuf[layer, side, q + r, m] * scale * norm_row[:, at : at + PIECE]).astype(BF16)

    def x_product(layer, size, n):
        x0s[8 : 8 + size, n * PIECE : (n + 1) * PIECE] = dot(hbuf[:size], wx[layer, n]).astype(BF16).astype(F32)

    def z_product(layer, size, n):
        zs[:size, n * PIECE : (n + 1) * PIECE] = jax.nn.silu(dot(hbuf[:size], wz[layer, n]).astype(BF16).astype(F32))

    def head(layer, q, subs, first, hook):
        size = subs * SUB
        if first:
            first_wait[0].wait()
        both = dot(hbuf[:size], wbd[layer]).astype(BF16).astype(F32)
        q0s[8 : 8 + size, :] = both[:, : 2 * HEAD]
        r_pre = both[:, 2 * HEAD : 2 * HEAD + 3 * (local // HEAD)]
        if first:
            for cp in smalls[1:-1]:
                cp.wait()
        if first:
            first_wait[1].wait()
        x_product(layer, size, 0)
        x_product(layer, size, 1)
        if not first:
            hook()
            x_product(layer, size, 2)
            x_product(layer, size, 3)
        bc = jax.nn.silu(tap_sum(q0s, size, slice(None), cbc[layer], row_of(bbc, layer)))
        q0s[0:8] = q0s[size : size + 8]
        triple = lambda ref: jnp.concatenate([row_of(ref, layer)] * 3, axis=1)
        dt_in = r_pre + triple(dtb)
        dt_val = jnp.maximum(dt_in, 0.0) + jnp.log1p(jnp.exp(-jnp.abs(dt_in)))
        a_vals = -dt_val * jnp.exp(triple(al))
        to_t, from_t = iota((size, 3 * size), 0), iota((size, 3 * size), 1) % size
        tri = jnp.where((to_t >= from_t) & (to_t // SUB == from_t // SUB), 1.0, 0.0).astype(BF16)
        a_cum = dot(tri, stack3(a_vals))
        skip = jnp.broadcast_to(triple(ds), (8, a_cum.shape[1]))
        to_spread = jnp.concatenate([dt_val, a_cum, skip], axis=0)
        hi, mid, lo = split3(to_spread)
        lane = iota(to_spread.shape, 1)
        n_heads = local // HEAD
        spread_in = jnp.where(lane < n_heads, hi, jnp.where(lane < 2 * n_heads, mid, lo)).astype(BF16)
        for n in range(n_piece):
            at = slice(n * PIECE, (n + 1) * PIECE)
            group = n * (PIECE // HEAD)
            pick = jnp.where(iota((3 * n_heads, PIECE), 1) // HEAD + group == iota((3 * n_heads, PIECE), 0) % n_heads, 1.0, 0.0).astype(BF16)
            spread[: 2 * size + 8, at] = dot(spread_in, pick)
        swapped = pltpu.roll(bc, HEAD, 1)
        turned = jnp.transpose(bc)
        c_stack, bt_stack, cb = [], [], []
        for r in range(subs):
            rows = slice(r * SUB, (r + 1) * SUB)
            c_stack.append(stack3(swapped[rows, :HEAD]))
            bt_stack.append(stack3(turned[:HEAD, rows]))
            cb.append(exact_dot(c_stack[r], [jnp.concatenate([part] * 4, axis=0).astype(BF16) for part in split3(bc[rows, :HEAD])], dot_nt))
        for r in range(subs):
            rows = slice(3 * r * SUB, 3 * (r + 1) * SUB)
            for n in range(n_piece):
                at = slice(n * PIECE, (n + 1) * PIECE)
                a_e = spread[size + r * SUB : size + (r + 1) * SUB, at]
                dstack[rows, at] = stack3(jnp.where(causal, jnp.exp(jnp.minimum(a_e - to_row(a_e), 0.0)), 0.0) * cb[r])

        def conv(n):
            at = slice(n * PIECE, (n + 1) * PIECE)
            xs[:size, at] = jax.nn.silu(tap_sum(x0s, size, at, cx[layer, :, at], row_of(bx, layer, at)))
            x0s[0:8, at] = x0s[size : size + 8, at]

        def inside(n):
            at = slice(n * PIECE, (n + 1) * PIECE)
            for r in range(subs):
                rows = slice(r * SUB, (r + 1) * SUB)
                x_dt = xs[rows, at] * spread[rows, at]
                ys[rows, at] = exact_dot(dstack[3 * r * SUB : 3 * (r + 1) * SUB, at], [head_blocks(part) for part in split3(x_dt)])

        def across(n):
            at = slice(n * PIECE, (n + 1) * PIECE)
            for r in range(subs):
                rows = slice(r * SUB, (r + 1) * SUB)
                a_e = spread[size + r * SUB : size + (r + 1) * SUB, at]
                a_last = a_e[SUB - 1 : SUB]
                old = state[:, at]
                carried = exact_dot(c_stack[r], [part.astype(BF16) for part in split3(old)])
                x_act = xs[rows, at]
                ys[rows, at] = ys[rows, at] + carried * jnp.exp(a_e) + spread[2 * size : 2 * size + 1, at] * x_act
                tail_x = x_act * spread[rows, at] * jnp.exp(a_last - a_e)
                state[:, at] = jnp.exp(a_last) * old + exact_dot(bt_stack[r], [part.astype(BF16) for part in split3(tail_x)])

        if first:
            conv(0)
            conv(1)
            first_wait[2].wait()
        plan = ORDER_FIRST if first else ORDER_LATER
        stages = {"x": lambda n: x_product(layer, size, n), "c": conv, "i": inside, "a": across, "z": lambda n: z_product(layer, size, n)}
        for step in plan:
            if step == "wait":
                first_wait[3].wait()
            else:
                stages[step[0]](int(step[1]))

    def tail(layer, q, subs, first):
        size = subs * SUB
        s = layer * n_subs + q
        gate_sq = jnp.zeros((size, 1), F32)
        for n in range(n_piece):
            at = slice(n * PIECE, (n + 1) * PIECE)
            v = ys[:size, at] * zs[:size, at]
            ys[:size, at] = v
            gate_sq = gate_sq + jnp.sum(v * v, axis=1, keepdims=True)
        scale = scale_of(gate_sq)
        gbuf[:size] = (ys[:size] * scale * row_of(gw, layer)).astype(BF16)
        for r in range(subs):
            pstat[core, s + r] = to_row(gate_sq[r * SUB : (r + 1) * SUB])[:, :128]
        if first:
            first_wait[4].wait()
        for m in range(n_piece):
            part = dot(gbuf[:size], wo[layer, 1 - core, m])
            for r in range(subs):
                psend[s + r, m] = part[r * SUB : (r + 1) * SUB]
        if first:
            pl.semaphore_wait(barrier, 2)
        for r in range(subs):
            pstat_copy(s + r).start()
            for m in range(n_piece):
                p_copy(s + r, m).start()
        if first:
            first_wait[5].wait()
        for m in range(n_piece):
            part = dot(gbuf[:size], wo[layer, core, m])
            for r in range(subs):
                own[m] = part[r * SUB : (r + 1) * SUB]

    def combine(s):
        pstat_copy(s).wait_recv()
        own_sq = to_col(pstat[core, s])
        peer_sq = to_col(pstat[1 - core, s])
        chip_sq = own_sq + peer_sq
        chip_scale = scale_of(chip_sq)
        f_own = chip_scale * inverse_of(own_sq)
        f_peer = chip_scale * inverse_of(peer_sq)
        qstat[chip, s] = to_row(chip_sq)[:, :128]
        qstat_copy(s).start()
        for m in range(n_piece):
            p_copy(s, m).wait_recv()
            qbuf[chip, s, m] = own[m] * f_own + prcv[s, m] * f_peer
            q_copy(s, m).start()

    def update(s, pieces=False):
        layer, c = s // n_subs, s % n_subs
        qstat_copy(s).wait_recv()
        if not pieces:
            q_arrived(s)
        sq0 = to_col(qstat[0, s])
        sq1 = to_col(qstat[1, s])
        norm = lax.rsqrt((sq0 + sq1) / inner + EPSILON)
        f0 = norm * inverse_of(sq0)
        f1 = norm * inverse_of(sq1)
        for m in range(n_piece):
            if pieces:
                q_copy(s, m).wait_recv()
            total = ubuf[layer, core, c, m] + (qbuf[0, s, m] * f0 + qbuf[1, s, m] * f1)
            ubuf[layer + 1, core, c, m] = total.astype(BF16).astype(F32)
            u_copy(s, m).start()

    def emit(s, pieces=False):
        c = s % n_subs
        for side in (core, 1 - core):
            if side is not core and not pieces:
                u_arrived(s)
            for m in range(n_piece):
                if side is not core and pieces:
                    u_copy(s, m).wait_recv()
                cols = pl.ds(pl.multiple_of(side * half + m * PIECE, PIECE), PIECE)
                out_ref[0, pl.ds(pl.multiple_of(c * SUB, SUB), SUB), cols] = ubuf[layers, side, c, m].astype(BF16)

    def load_hidden(c):
        hid_copy(c).wait()
        for side in range(2):
            for m in range(n_piece):
                at = side * half + m * PIECE
                ubuf[0, side, c, m] = hid[c, :, at : at + PIECE].astype(F32)

    steps = layers * n_subs
    lag = n_subs - 1
    steps = layers * n_subs
    lag = n_subs - 1
    start_layer()
    smalls[0].wait()
    smalls[-1].wait()
    turn_wdt(0)
    load_hidden(0)
    norm(0, 0, 1)
    head(0, 0, 1, True, lambda: None)
    tail(0, 0, 1, True)

    bc_copy(1).start()
    start_weights(1)
    combine(0)

    @pl.loop(1, steps)
    def _(t):
        layer, q = t // n_subs, t % n_subs

        @pl.when(t < n_subs)
        def _():
            load_hidden(q)

        @pl.when(t >= n_subs)
        def _():
            u_arrived(t - n_subs)

        for at in range(1, layers):
            @pl.when(t == at * n_subs)
            def _():
                start_layer()
                turn_wdt(at)
                for cp in weight_waits(at):
                    cp.wait()
                if at + 1 < layers:
                    bc_copy(at + 1).start()
                    start_weights(at + 1)

        norm(layer, q, 1)

        @pl.when(t == 2)
        def _():
            combine(t - 1)

        @pl.when(t >= lag)
        def _():
            update(t - lag)

        def hook():
            @pl.when(t > 2)
            def _():
                combine(t - 1)

        head(layer, q, 1, False, hook)
        tail(layer, q, 1, False)

    combine(steps - 1)
    final = steps - n_subs

    @pl.loop(final, steps - 1)
    def _(s):
        @pl.when(s > final)
        def _():
            emit(s - 1)

        @pl.when(s > steps - 1 - lag)
        def _():
            update(s)

    emit(steps - 2)
    update(steps - 1, True)
    emit(steps - 1, True)
    all_sent()


def solution(mesh):
    in_specs = (P('dp'), P(), P(None, None, 'tp'), P(None, None, 'tp'), P(), P(None, None, 'tp'), P(None, None, 'tp'), P(), P(None, 'tp'), P(),
                P(None, 'tp'), P(None, 'tp'), P(None, 'tp'), P(None, 'tp'), P(None, 'tp', None))
    tp_size = mesh.shape['tp']

    def device_forward(hidden, norm_w, w_z, w_x, w_bc, w_dt, conv_x, conv_bc, bias_x, bias_bc, dt_bias, a_log, d_skip, gate_w, w_out):
        layers, width, local = w_x.shape
        n_subs = hidden.shape[1] // SUB
        n_piece = local // PIECE
        steps = layers * n_subs
        bc_width = w_bc.shape[-1]
        w_dt = jnp.swapaxes(w_dt, 1, 2)
        vm = lambda shape, dtype: pltpu.VMEM(shape, dtype)
        same = lambda arr: pltpu.VMEM(arr.shape, arr.dtype)
        scratch = [
            vm((n_subs, SUB, width), BF16), same(norm_w), vm((layers, n_piece, width, PIECE), BF16), vm((layers, n_piece, width, PIECE), BF16),
            vm((layers, width, PIECE), BF16), same(w_dt), same(conv_x), same(conv_bc), same(bias_x), same(bias_bc), same(dt_bias), same(a_log), same(d_skip), same(gate_w),
            vm((layers, 2, n_piece, local, PIECE), BF16),
            vm((layers + 1, 2, n_subs, n_piece, SUB, PIECE), F32),
            vm((steps, n_piece, SUB, PIECE), F32), vm((steps, n_piece, SUB, PIECE), F32), vm((2, steps, n_piece, SUB, PIECE), F32),
            vm((2, steps, 1, 128), F32), vm((2, steps, 1, 128), F32),
            vm((n_piece, SUB, PIECE), F32), vm((MAX_ROWS, width), BF16), vm((MAX_ROWS + 8, local), F32), vm((MAX_ROWS + 8, bc_width), F32),
            vm((MAX_ROWS, local), F32), vm((MAX_ROWS, local), F32), vm((MAX_ROWS, local), F32), vm((3 * MAX_ROWS, local), BF16), vm((2 * MAX_ROWS + 8, local), F32), vm((HEAD, local), F32), vm((MAX_ROWS, local), BF16),
            pltpu.SemaphoreType.DMA((10,)), pltpu.SemaphoreType.DMA((n_subs,)), pltpu.SemaphoreType.DMA((6,)), pltpu.SemaphoreType.DMA((5,)),
            pltpu.SemaphoreType.DMA((2, n_piece)), pltpu.SemaphoreType.DMA((steps - 1 + n_piece,)), pltpu.SemaphoreType.DMA((steps - 1 + n_piece,)),
            pltpu.SemaphoreType.DMA((2,)), pltpu.SemaphoreType.DMA((steps,)),
        ]
        return pl.pallas_call(
            functools.partial(kernel, float(local * tp_size)),
            out_shape=jax.ShapeDtypeStruct(hidden.shape, hidden.dtype),
            in_specs=[pl.BlockSpec(memory_space=pltpu.HBM)] * 15,
            out_specs=pl.BlockSpec(memory_space=pltpu.VMEM),
            scratch_shapes=scratch,
            compiler_params=pltpu.CompilerParams(collective_id=0, has_side_effects=True, vmem_limit_bytes=52 * 1024 * 1024),
        )(*[pltpu.with_memory_space_constraint(arr, pltpu.HBM) for arr in (hidden, norm_w, w_z, w_x, w_bc, w_dt, conv_x, conv_bc, bias_x, bias_bc, dt_bias, a_log, d_skip, gate_w, w_out)])

    return jax.shard_map(device_forward, mesh=mesh, in_specs=in_specs, out_specs=P('dp'), check_vma=False)
```

```python
import functools

import jax
import jax.numpy as jnp
from jax import lax
from jax.experimental import pallas as pl
from jax.experimental.pallas import tpu as pltpu
from jax.sharding import PartitionSpec as P

EPSILON = 1e-5
MESH = pl.DeviceIdType.MESH
SUB = 64
MAX_ROWS = 64
ORDER_FIRST = ("x2", "i0", "x3", "i1", "c2", "a0", "c3", "a1", "i2", "a2", "i3", "a3", "wait", "z0", "z1", "z2", "z3")
ORDER_LATER = ("c0", "z0", "c1", "i0", "c2", "z1", "i1", "a0", "c3", "z2", "i2", "a1", "z3", "i3", "a2", "a3")
PIECE = 256
HEAD = 64
F32 = jnp.float32
BF16 = jnp.bfloat16


def split3(val):
    hi = val.astype(BF16).astype(F32)
    rest = val - hi
    mid = rest.astype(BF16).astype(F32)
    return hi, mid, rest - mid


def stack3(val):
    return jnp.concatenate(split3(val), axis=0).astype(BF16)


def dot(a, b):
    return lax.dot_general(a, b, (((1,), (0,)), ((), ())), preferred_element_type=F32)


def dot_nt(a, b):
    return lax.dot_general(a, b, (((1,), (1,)), ((), ())), preferred_element_type=F32)


def exact_dot(a_stack, b_parts, product=dot):
    rows = a_stack.shape[0] // 3
    b_hi, b_mid, b_lo = b_parts
    r1 = product(a_stack, b_hi)
    r2 = product(a_stack[: 2 * rows], b_mid)
    r3 = product(a_stack[:rows], b_lo)
    small = r1[2 * rows :] + r2[rows:] + r3
    return r1[:rows] + (r1[rows : 2 * rows] + r2[:rows] + small)


def iota(shape, dim):
    return lax.broadcasted_iota(jnp.int32, shape, dim)


def kernel(inner, hid_h, nw_h, wz_h, wx_h, wbc_h, wdt_h, cx_h, cbc_h, bx_h, bbc_h, dtb_h, al_h, ds_h, gw_h, wo_h,
           out_ref, hid, nw, wz, wx, wbd, wdt, cx, cbc, bx, bbc, dtb, al, ds, gw, wo,
           ubuf, psend, prcv, qbuf, pstat, qstat, own, hbuf, x0s, q0s, xs, ys, zs, dstack, spread, state, gbuf,
           small_sem, hid_sem, w_sem, send_sem, pr_sem, qr_sem, ur_sem, ptr_sem, qtr_sem):
    me = lax.axis_index("tp")
    core = me % 2
    chip = me // 2
    peer = me + 1 - 2 * core
    cross = (me + 2) % 4
    n_subs = hid_h.shape[1] // SUB
    n_piece = wx_h.shape[2] // PIECE
    layers = nw_h.shape[0]
    local = wx_h.shape[2]
    half = wo_h.shape[2] // 2

    barrier = pltpu.get_barrier_semaphore()
    for other in (peer, cross):
        pl.semaphore_signal(barrier, inc=1, device_id={"tp": other}, device_id_type=MESH)

    smalls = [pltpu.make_async_copy(src, dst, small_sem.at[i]) for i, (src, dst) in enumerate(
        [(nw_h, nw), (cx_h, cx), (cbc_h, cbc), (bx_h, bx), (bbc_h, bbc), (dtb_h, dtb), (al_h, al), (ds_h, ds), (gw_h, gw), (wdt_h, wdt)])]

    def hid_copy(c):
        return pltpu.make_async_copy(hid_h.at[0, pl.ds(c * SUB, SUB)], hid.at[c], hid_sem.at[c])

    def start_weights(layer):
        cols = lambda n: pl.ds(pl.multiple_of(n * PIECE, PIECE), PIECE)

        @pl.loop(0, n_piece)
        def _(n):
            pltpu.make_async_copy(wx_h.at[layer, :, cols(n)], wx.at[layer, n], w_sem.at[1 + n // 2]).start()

        @pl.loop(0, n_piece)
        def _(n):
            pltpu.make_async_copy(wz_h.at[layer, :, cols(n)], wz.at[layer, n], w_sem.at[3]).start()

        @pl.loop(0, 2 * n_piece)
        def _(n):
            side = (n // n_piece + 1 - core) % 2
            pltpu.make_async_copy(wo_h.at[layer, :, cols(side * n_piece + n % n_piece)], wo.at[layer, side, n % n_piece], w_sem.at[4 + n // n_piece]).start()

    def bc_copy(layer):
        return pltpu.make_async_copy(wbc_h.at[layer], wbd.at[layer, :, pl.ds(0, 2 * HEAD)], w_sem.at[0])

    def weight_waits(layer):
        whole = lambda ref, sem: pltpu.make_async_copy(ref, ref, w_sem.at[sem])
        return [whole(wbd.at[layer, :, pl.ds(0, 2 * HEAD)], 0), whole(wx.at[layer, pl.ds(0, 2)], 1), whole(wx.at[layer, pl.ds(2, 2)], 2), whole(wz.at[layer], 3), whole(wo.at[layer, 1 - core], 4), whole(wo.at[layer, core], 5)]

    first_wait = weight_waits(0)
    for cp in [smalls[0], smalls[-1], hid_copy(0), bc_copy(0)] + smalls[1:-1]:
        cp.start()
    start_weights(0)
    for q in range(1, n_subs):
        hid_copy(q).start()

    def remote(src, dst, sem, recv_sem, target):
        return pltpu.make_async_remote_copy(src_ref=src, dst_ref=dst, send_sem=send_sem.at[sem], recv_sem=recv_sem, device_id={"tp": target}, device_id_type=MESH)

    last = layers * n_subs - 1

    def own_slot(s, m):
        return s + m * (s // last)

    def p_copy(s, m):
        return remote(psend.at[s, m], prcv.at[s, m], 0, pr_sem.at[s % 2, m], peer)

    def pstat_copy(s):
        return remote(pstat.at[core, s], pstat.at[core, s], 1, ptr_sem.at[s % 2], peer)

    def q_copy(s, m):
        return remote(qbuf.at[chip, s, m], qbuf.at[chip, s, m], 2, qr_sem.at[own_slot(s, m)], cross)

    def qstat_copy(s):
        return remote(qstat.at[chip, s], qstat.at[chip, s], 3, qtr_sem.at[s], cross)

    def u_copy(s, m):
        spot = ubuf.at[s // n_subs + 1, core, s % n_subs, m]
        return remote(spot, spot, 4, ur_sem.at[own_slot(s, m)], peer)

    def q_arrived(s):
        remote(qbuf.at[chip, s], qbuf.at[chip, s], 2, qr_sem.at[s], cross).wait_recv()

    def u_arrived(s):
        spot = ubuf.at[s // n_subs + 1, core, s % n_subs]
        remote(spot, spot, 4, ur_sem.at[s], peer).wait_recv()

    def all_sent():
        shared = ubuf.at[pl.ds(1, layers), core]
        for sem, ref in enumerate((psend, pstat.at[core], qbuf.at[chip], qstat.at[chip], shared)):
            remote(ref, ref, sem, qtr_sem.at[0], cross).wait_send()

    row64 = iota((SUB, PIECE), 0)
    lane64 = iota((SUB, PIECE), 1) % HEAD
    eye = row64 == lane64
    causal = row64 >= lane64
    low_head = iota((SUB, 128), 1) < HEAD

    def to_row(col):
        return jnp.sum(jnp.where(eye, col, 0.0), axis=0, keepdims=True)

    def to_col(row):
        return jnp.sum(jnp.where(eye[:, :HEAD], row[:, :HEAD], 0.0), axis=1, keepdims=True)

    def scale_of(square_sum):
        return lax.rsqrt(square_sum / inner + EPSILON) * (1.0 / 64.0)

    def inverse_of(square_sum):
        return jnp.where(square_sum < jnp.inf, 64.0 * jnp.sqrt(square_sum / inner + EPSILON), 0.0)

    def head_blocks(part):
        left, right = part[:, :128], part[:, 128:]
        none = jnp.zeros_like(left)
        rows = [jnp.concatenate([jnp.where(low_head, left, 0.0), none], axis=1), jnp.concatenate([jnp.where(low_head, 0.0, left), none], axis=1),
                jnp.concatenate([none, jnp.where(low_head, right, 0.0)], axis=1), jnp.concatenate([none, jnp.where(low_head, 0.0, right)], axis=1)]
        return jnp.concatenate(rows, axis=0).astype(BF16)

    def row_of(ref, layer, lanes=slice(None)):
        row = ref[0:1, lanes]
        for at in range(1, layers):
            row = jnp.where(layer == at, ref[at : at + 1, lanes], row)
        return row.astype(F32)

    def turn_wdt(layer):
        for k in range(0, wdt.shape[2], 128):
            block = wdt[layer, :, k : k + 128].astype(F32)
            turned = jnp.transpose(jnp.concatenate([block] * 3, axis=0)).astype(BF16)
            wbd[layer, k : k + 128, 2 * HEAD : 2 * HEAD + turned.shape[1]] = turned

    def start_layer():
        state[...] = jnp.zeros_like(state)
        x0s[0:8] = jnp.zeros((8, local), F32)
        q0s[0:8] = jnp.zeros((8, q0s.shape[1]), F32)

    def tap_sum(buf, size, lanes, kern, bias):
        total = bias
        for j in range(4):
            total = total + buf[5 + j : 5 + j + size, lanes] * kern[j : j + 1].astype(F32)
        return total

    def norm(layer, q, subs):
        square = [jnp.zeros((SUB, 1), F32) for _ in range(subs)]
        for r in range(subs):
            for side in range(2):
                for m in range(n_piece):
                    val = ubuf[layer, side, q + r, m]
                    square[r] = square[r] + jnp.sum(val * val, axis=1, keepdims=True)
        norm_row = row_of(nw, layer)
        for r in range(subs):
            scale = lax.rsqrt(square[r] / (2 * half) + EPSILON)
            for side in range(2):
                for m in range(n_piece):
                    at = side * half + m * PIECE
                    hbuf[r * SUB : (r + 1) * SUB, at : at + PIECE] = (ubuf[layer, side, q + r, m] * scale * norm_row[:, at : at + PIECE]).astype(BF16)

    def x_product(layer, size, n):
        x0s[8 : 8 + size, n * PIECE : (n + 1) * PIECE] = dot(hbuf[:size], wx[layer, n]).astype(BF16).astype(F32)

    def z_product(layer, size, n):
        zs[:size, n * PIECE : (n + 1) * PIECE] = jax.nn.silu(dot(hbuf[:size], wz[layer, n]).astype(BF16).astype(F32))

    def head(layer, q, subs, first, hook):
        size = subs * SUB
        if first:
            first_wait[0].wait()
        both = dot(hbuf[:size], wbd[layer]).astype(BF16).astype(F32)
        q0s[8 : 8 + size, :] = both[:, : 2 * HEAD]
        r_pre = both[:, 2 * HEAD : 2 * HEAD + 3 * (local // HEAD)]
        if first:
            for cp in smalls[1:-1]:
                cp.wait()
        if first:
            first_wait[1].wait()
        x_product(layer, size, 0)
        x_product(layer, size, 1)
        if not first:
            hook()
            x_product(layer, size, 2)
            x_product(layer, size, 3)
        bc = jax.nn.silu(tap_sum(q0s, size, slice(None), cbc[layer], row_of(bbc, layer)))
        q0s[0:8] = q0s[size : size + 8]
        triple = lambda ref: jnp.concatenate([row_of(ref, layer)] * 3, axis=1)
        dt_in = r_pre + triple(dtb)
        dt_val = jnp.maximum(dt_in, 0.0) + jnp.log1p(jnp.exp(-jnp.abs(dt_in)))
        a_vals = -dt_val * jnp.exp(triple(al))
        to_t, from_t = iota((size, 3 * size), 0), iota((size, 3 * size), 1) % size
        tri = jnp.where((to_t >= from_t) & (to_t // SUB == from_t // SUB), 1.0, 0.0).astype(BF16)
        a_cum = dot(tri, stack3(a_vals))
        skip = jnp.broadcast_to(triple(ds), (8, a_cum.shape[1]))
        to_spread = jnp.concatenate([dt_val, a_cum, skip], axis=0)
        hi, mid, lo = split3(to_spread)
        lane = iota(to_spread.shape, 1)
        n_heads = local // HEAD
        spread_in = jnp.where(lane < n_heads, hi, jnp.where(lane < 2 * n_heads, mid, lo)).astype(BF16)
        for n in range(n_piece):
            at = slice(n * PIECE, (n + 1) * PIECE)
            group = n * (PIECE // HEAD)
            pick = jnp.where(iota((3 * n_heads, PIECE), 1) // HEAD + group == iota((3 * n_heads, PIECE), 0) % n_heads, 1.0, 0.0).astype(BF16)
            spread[: 2 * size + 8, at] = dot(spread_in, pick)
        swapped = pltpu.roll(bc, HEAD, 1)
        turned = jnp.transpose(bc)
        c_stack, bt_stack, cb = [], [], []
        for r in range(subs):
            rows = slice(r * SUB, (r + 1) * SUB)
            c_stack.append(stack3(swapped[rows, :HEAD]))
            bt_stack.append(stack3(turned[:HEAD, rows]))
            cb.append(exact_dot(c_stack[r], [jnp.concatenate([part] * 4, axis=0).astype(BF16) for part in split3(bc[rows, :HEAD])], dot_nt))
        for r in range(subs):
            rows = slice(3 * r * SUB, 3 * (r + 1) * SUB)
            for n in range(n_piece):
                at = slice(n * PIECE, (n + 1) * PIECE)
                a_e = spread[size + r * SUB : size + (r + 1) * SUB, at]
                dstack[rows, at] = stack3(jnp.where(causal, jnp.exp(jnp.minimum(a_e - to_row(a_e), 0.0)), 0.0) * cb[r])

        def conv(n):
            at = slice(n * PIECE, (n + 1) * PIECE)
            xs[:size, at] = jax.nn.silu(tap_sum(x0s, size, at, cx[layer, :, at], row_of(bx, layer, at)))
            x0s[0:8, at] = x0s[size : size + 8, at]

        def inside(n):
            at = slice(n * PIECE, (n + 1) * PIECE)
            for r in range(subs):
                rows = slice(r * SUB, (r + 1) * SUB)
                x_dt = xs[rows, at] * spread[rows, at]
                ys[rows, at] = exact_dot(dstack[3 * r * SUB : 3 * (r + 1) * SUB, at], [head_blocks(part) for part in split3(x_dt)])

        def across(n):
            at = slice(n * PIECE, (n + 1) * PIECE)
            for r in range(subs):
                rows = slice(r * SUB, (r + 1) * SUB)
                a_e = spread[size + r * SUB : size + (r + 1) * SUB, at]
                a_last = a_e[SUB - 1 : SUB]
                old = state[:, at]
                carried = exact_dot(c_stack[r], [part.astype(BF16) for part in split3(old)])
                x_act = xs[rows, at]
                ys[rows, at] = ys[rows, at] + carried * jnp.exp(a_e) + spread[2 * size : 2 * size + 1, at] * x_act
                tail_x = x_act * spread[rows, at] * jnp.exp(a_last - a_e)
                state[:, at] = jnp.exp(a_last) * old + exact_dot(bt_stack[r], [part.astype(BF16) for part in split3(tail_x)])

        if first:
            conv(0)
            conv(1)
            first_wait[2].wait()
        plan = ORDER_FIRST if first else ORDER_LATER
        stages = {"x": lambda n: x_product(layer, size, n), "c": conv, "i": inside, "a": across, "z": lambda n: z_product(layer, size, n)}
        for step in plan:
            if step == "wait":
                first_wait[3].wait()
            else:
                stages[step[0]](int(step[1]))

    def tail(layer, q, subs, first):
        size = subs * SUB
        s = layer * n_subs + q
        gate_sq = jnp.zeros((size, 1), F32)
        for n in range(n_piece):
            at = slice(n * PIECE, (n + 1) * PIECE)
            v = ys[:size, at] * zs[:size, at]
            ys[:size, at] = v
            gate_sq = gate_sq + jnp.sum(v * v, axis=1, keepdims=True)
        scale = scale_of(gate_sq)
        gbuf[:size] = (ys[:size] * scale * row_of(gw, layer)).astype(BF16)
        for r in range(subs):
            pstat[core, s + r] = to_row(gate_sq[r * SUB : (r + 1) * SUB])[:, :128]
        if first:
            first_wait[4].wait()
        groups = [range(n_piece // 2), range(n_piece // 2, n_piece)] if first else [range(n_piece)]
        for pieces in groups:
            for m in pieces:
                part = dot(gbuf[:size], wo[layer, 1 - core, m])
                for r in range(subs):
                    psend[s + r, m] = part[r * SUB : (r + 1) * SUB]
            if first and pieces[0] == 0:
                pl.semaphore_wait(barrier, 2)
            for r in range(subs):
                if pieces[0] == 0:
                    pstat_copy(s + r).start()
                for m in pieces:
                    p_copy(s + r, m).start()
        if first:
            first_wait[5].wait()
        for m in range(n_piece):
            part = dot(gbuf[:size], wo[layer, core, m])
            for r in range(subs):
                own[m] = part[r * SUB : (r + 1) * SUB]

    def combine(s):
        pstat_copy(s).wait_recv()
        own_sq = to_col(pstat[core, s])
        peer_sq = to_col(pstat[1 - core, s])
        chip_sq = own_sq + peer_sq
        chip_scale = scale_of(chip_sq)
        f_own = chip_scale * inverse_of(own_sq)
        f_peer = chip_scale * inverse_of(peer_sq)
        qstat[chip, s] = to_row(chip_sq)[:, :128]
        qstat_copy(s).start()
        for m in range(n_piece):
            p_copy(s, m).wait_recv()
            qbuf[chip, s, m] = own[m] * f_own + prcv[s, m] * f_peer
            q_copy(s, m).start()

    def update(s, pieces=False):
        layer, c = s // n_subs, s % n_subs
        qstat_copy(s).wait_recv()
        if not pieces:
            q_arrived(s)
        sq0 = to_col(qstat[0, s])
        sq1 = to_col(qstat[1, s])
        norm = lax.rsqrt((sq0 + sq1) / inner + EPSILON)
        f0 = norm * inverse_of(sq0)
        f1 = norm * inverse_of(sq1)
        for m in range(n_piece):
            if pieces:
                q_copy(s, m).wait_recv()
            total = ubuf[layer, core, c, m] + (qbuf[0, s, m] * f0 + qbuf[1, s, m] * f1)
            ubuf[layer + 1, core, c, m] = total.astype(BF16).astype(F32)
            u_copy(s, m).start()

    def emit(s, pieces=False):
        c = s % n_subs
        for side in (core, 1 - core):
            if side is not core and not pieces:
                u_arrived(s)
            for m in range(n_piece):
                if side is not core and pieces:
                    u_copy(s, m).wait_recv()
                cols = pl.ds(pl.multiple_of(side * half + m * PIECE, PIECE), PIECE)
                out_ref[0, pl.ds(pl.multiple_of(c * SUB, SUB), SUB), cols] = ubuf[layers, side, c, m].astype(BF16)

    def load_hidden(c):
        hid_copy(c).wait()
        for side in range(2):
            for m in range(n_piece):
                at = side * half + m * PIECE
                ubuf[0, side, c, m] = hid[c, :, at : at + PIECE].astype(F32)

    steps = layers * n_subs
    lag = n_subs - 1
    steps = layers * n_subs
    lag = n_subs - 1
    start_layer()
    smalls[0].wait()
    smalls[-1].wait()
    turn_wdt(0)
    load_hidden(0)
    norm(0, 0, 1)
    head(0, 0, 1, True, lambda: None)
    tail(0, 0, 1, True)

    bc_copy(1).start()
    start_weights(1)
    combine(0)

    @pl.loop(1, steps)
    def _(t):
        layer, q = t // n_subs, t % n_subs

        @pl.when(t < n_subs)
        def _():
            load_hidden(q)

        @pl.when(t >= n_subs)
        def _():
            u_arrived(t - n_subs)

        for at in range(1, layers):
            @pl.when(t == at * n_subs)
            def _():
                start_layer()
                turn_wdt(at)
                for cp in weight_waits(at):
                    cp.wait()
                if at + 1 < layers:
                    bc_copy(at + 1).start()
                    start_weights(at + 1)

        norm(layer, q, 1)

        @pl.when(t == 2)
        def _():
            combine(t - 1)

        @pl.when(t >= lag)
        def _():
            update(t - lag)

        def hook():
            @pl.when(t > 2)
            def _():
                combine(t - 1)

        head(layer, q, 1, False, hook)
        tail(layer, q, 1, False)

    combine(steps - 1)
    final = steps - n_subs

    @pl.loop(final, steps - 1)
    def _(s):
        @pl.when(s > final)
        def _():
            emit(s - 1)

        @pl.when(s > steps - 1 - lag)
        def _():
            update(s)

    emit(steps - 2)
    update(steps - 1, True)
    emit(steps - 1, True)
    all_sent()


def solution(mesh):
    in_specs = (P('dp'), P(), P(None, None, 'tp'), P(None, None, 'tp'), P(), P(None, None, 'tp'), P(None, None, 'tp'), P(), P(None, 'tp'), P(),
                P(None, 'tp'), P(None, 'tp'), P(None, 'tp'), P(None, 'tp'), P(None, 'tp', None))
    tp_size = mesh.shape['tp']

    def device_forward(hidden, norm_w, w_z, w_x, w_bc, w_dt, conv_x, conv_bc, bias_x, bias_bc, dt_bias, a_log, d_skip, gate_w, w_out):
        layers, width, local = w_x.shape
        n_subs = hidden.shape[1] // SUB
        n_piece = local // PIECE
        steps = layers * n_subs
        bc_width = w_bc.shape[-1]
        w_dt = jnp.swapaxes(w_dt, 1, 2)
        vm = lambda shape, dtype: pltpu.VMEM(shape, dtype)
        same = lambda arr: pltpu.VMEM(arr.shape, arr.dtype)
        scratch = [
            vm((n_subs, SUB, width), BF16), same(norm_w), vm((layers, n_piece, width, PIECE), BF16), vm((layers, n_piece, width, PIECE), BF16),
            vm((layers, width, PIECE), BF16), same(w_dt), same(conv_x), same(conv_bc), same(bias_x), same(bias_bc), same(dt_bias), same(a_log), same(d_skip), same(gate_w),
            vm((layers, 2, n_piece, local, PIECE), BF16),
            vm((layers + 1, 2, n_subs, n_piece, SUB, PIECE), F32),
            vm((steps, n_piece, SUB, PIECE), F32), vm((steps, n_piece, SUB, PIECE), F32), vm((2, steps, n_piece, SUB, PIECE), F32),
            vm((2, steps, 1, 128), F32), vm((2, steps, 1, 128), F32),
            vm((n_piece, SUB, PIECE), F32), vm((MAX_ROWS, width), BF16), vm((MAX_ROWS + 8, local), F32), vm((MAX_ROWS + 8, bc_width), F32),
            vm((MAX_ROWS, local), F32), vm((MAX_ROWS, local), F32), vm((MAX_ROWS, local), F32), vm((3 * MAX_ROWS, local), BF16), vm((2 * MAX_ROWS + 8, local), F32), vm((HEAD, local), F32), vm((MAX_ROWS, local), BF16),
            pltpu.SemaphoreType.DMA((10,)), pltpu.SemaphoreType.DMA((n_subs,)), pltpu.SemaphoreType.DMA((6,)), pltpu.SemaphoreType.DMA((5,)),
            pltpu.SemaphoreType.DMA((2, n_piece)), pltpu.SemaphoreType.DMA((steps - 1 + n_piece,)), pltpu.SemaphoreType.DMA((steps - 1 + n_piece,)),
            pltpu.SemaphoreType.DMA((2,)), pltpu.SemaphoreType.DMA((steps,)),
        ]
        return pl.pallas_call(
            functools.partial(kernel, float(local * tp_size)),
            out_shape=jax.ShapeDtypeStruct(hidden.shape, hidden.dtype),
            in_specs=[pl.BlockSpec(memory_space=pltpu.HBM)] * 15,
            out_specs=pl.BlockSpec(memory_space=pltpu.VMEM),
            scratch_shapes=scratch,
            compiler_params=pltpu.CompilerParams(collective_id=0, has_side_effects=True, vmem_limit_bytes=52 * 1024 * 1024),
        )(*[pltpu.with_memory_space_constraint(arr, pltpu.HBM) for arr in (hidden, norm_w, w_z, w_x, w_bc, w_dt, conv_x, conv_bc, bias_x, bias_bc, dt_bias, a_log, d_skip, gate_w, w_out)])

    return jax.shard_map(device_forward, mesh=mesh, in_specs=in_specs, out_specs=P('dp'), check_vma=False)
```

```python
import functools

import jax
import jax.numpy as jnp
from jax import lax
from jax.experimental import pallas as pl
from jax.experimental.pallas import tpu as pltpu
from jax.sharding import PartitionSpec as P

EPSILON = 1e-5
MESH = pl.DeviceIdType.MESH
SUB = 64
MAX_ROWS = 64
ORDER_FIRST = ("x2", "i0", "x3", "i1", "c2", "a0", "c3", "a1", "i2", "a2", "i3", "a3", "wait", "z0", "z1", "z2", "z3")
ORDER_LATER = ("c0", "z0", "c1", "i0", "c2", "z1", "i1", "a0", "c3", "z2", "i2", "a1", "z3", "i3", "a2", "a3")
PIECE = 256
HEAD = 64
F32 = jnp.float32
BF16 = jnp.bfloat16


def split3(val):
    hi = val.astype(BF16).astype(F32)
    rest = val - hi
    mid = rest.astype(BF16).astype(F32)
    return hi, mid, rest - mid


def stack3(val):
    return jnp.concatenate(split3(val), axis=0).astype(BF16)


def dot(a, b):
    return lax.dot_general(a, b, (((1,), (0,)), ((), ())), preferred_element_type=F32)


def dot_nt(a, b):
    return lax.dot_general(a, b, (((1,), (1,)), ((), ())), preferred_element_type=F32)


def exact_dot(a_stack, b_parts, product=dot):
    rows = a_stack.shape[0] // 3
    b_hi, b_mid, b_lo = b_parts
    r1 = product(a_stack, b_hi)
    r2 = product(a_stack[: 2 * rows], b_mid)
    r3 = product(a_stack[:rows], b_lo)
    small = r1[2 * rows :] + r2[rows:] + r3
    return r1[:rows] + (r1[rows : 2 * rows] + r2[:rows] + small)


def iota(shape, dim):
    return lax.broadcasted_iota(jnp.int32, shape, dim)


def kernel(inner, hid_h, nw_h, wz_h, wx_h, wbc_h, wdt_h, cx_h, cbc_h, bx_h, bbc_h, dtb_h, al_h, ds_h, gw_h, wo_h,
           out_ref, hid, nw, wz, wx, wbd, wdt, cx, cbc, bx, bbc, dtb, al, ds, gw, wo,
           ubuf, psend, prcv, qbuf, pstat, qstat, own, hbuf, x0s, q0s, xs, ys, zs, dstack, spread, state, gbuf,
           small_sem, hid_sem, w_sem, send_sem, pr_sem, qr_sem, ur_sem, ptr_sem, qtr_sem):
    me = lax.axis_index("tp")
    core = me % 2
    chip = me // 2
    peer = me + 1 - 2 * core
    cross = (me + 2) % 4
    n_subs = hid_h.shape[1] // SUB
    n_piece = wx_h.shape[2] // PIECE
    layers = nw_h.shape[0]
    local = wx_h.shape[2]
    half = wo_h.shape[2] // 2

    barrier = pltpu.get_barrier_semaphore()
    for other in (peer, cross):
        pl.semaphore_signal(barrier, inc=1, device_id={"tp": other}, device_id_type=MESH)

    smalls = [pltpu.make_async_copy(src, dst, small_sem.at[i]) for i, (src, dst) in enumerate(
        [(nw_h, nw), (cx_h, cx), (cbc_h, cbc), (bx_h, bx), (bbc_h, bbc), (dtb_h, dtb), (al_h, al), (ds_h, ds), (gw_h, gw), (wdt_h, wdt)])]

    def hid_copy(c):
        return pltpu.make_async_copy(hid_h.at[0, pl.ds(c * SUB, SUB)], hid.at[c], hid_sem.at[c])

    def start_weights(layer):
        cols = lambda n: pl.ds(pl.multiple_of(n * PIECE, PIECE), PIECE)

        @pl.loop(0, n_piece)
        def _(n):
            pltpu.make_async_copy(wx_h.at[layer, :, cols(n)], wx.at[layer, n], w_sem.at[1 + n // 2]).start()

        @pl.loop(0, n_piece)
        def _(n):
            pltpu.make_async_copy(wz_h.at[layer, :, cols(n)], wz.at[layer, n], w_sem.at[3]).start()

        @pl.loop(0, 2 * n_piece)
        def _(n):
            side = (n // n_piece + 1 - core) % 2
            pltpu.make_async_copy(wo_h.at[layer, :, cols(side * n_piece + n % n_piece)], wo.at[layer, side, n % n_piece], w_sem.at[4 + n // n_piece]).start()

    def bc_copy(layer):
        return pltpu.make_async_copy(wbc_h.at[layer], wbd.at[layer, :, pl.ds(0, 2 * HEAD)], w_sem.at[0])

    def weight_waits(layer):
        whole = lambda ref, sem: pltpu.make_async_copy(ref, ref, w_sem.at[sem])
        return [whole(wbd.at[layer, :, pl.ds(0, 2 * HEAD)], 0), whole(wx.at[layer, pl.ds(0, 2)], 1), whole(wx.at[layer, pl.ds(2, 2)], 2), whole(wz.at[layer], 3), whole(wo.at[layer, 1 - core], 4), whole(wo.at[layer, core], 5)]

    first_wait = weight_waits(0)
    for cp in [smalls[0], smalls[-1], hid_copy(0), bc_copy(0)] + smalls[1:-1]:
        cp.start()
    start_weights(0)
    for q in range(1, n_subs):
        hid_copy(q).start()

    def remote(src, dst, sem, recv_sem, target):
        return pltpu.make_async_remote_copy(src_ref=src, dst_ref=dst, send_sem=send_sem.at[sem], recv_sem=recv_sem, device_id={"tp": target}, device_id_type=MESH)

    last = layers * n_subs - 1

    def own_slot(s, m):
        return s + m * (s // last)

    def p_copy(s, m):
        return remote(psend.at[s, m], prcv.at[s, m], 0, pr_sem.at[s % 2, m // 2], peer)

    def pstat_copy(s):
        return remote(pstat.at[core, s], pstat.at[core, s], 1, ptr_sem.at[s % 2], peer)

    def q_copy(s, m):
        return remote(qbuf.at[chip, s, m], qbuf.at[chip, s, m], 2, qr_sem.at[own_slot(s, m)], cross)

    def qstat_copy(s):
        return remote(qstat.at[chip, s], qstat.at[chip, s], 3, qtr_sem.at[s], cross)

    def u_copy(s, m):
        spot = ubuf.at[s // n_subs + 1, core, s % n_subs, m]
        return remote(spot, spot, 4, ur_sem.at[own_slot(s, m)], peer)

    def q_arrived(s):
        remote(qbuf.at[chip, s], qbuf.at[chip, s], 2, qr_sem.at[s], cross).wait_recv()

    def u_arrived(s):
        spot = ubuf.at[s // n_subs + 1, core, s % n_subs]
        remote(spot, spot, 4, ur_sem.at[s], peer).wait_recv()

    def all_sent():
        shared = ubuf.at[pl.ds(1, layers), core]
        for sem, ref in enumerate((psend, pstat.at[core], qbuf.at[chip], qstat.at[chip], shared)):
            remote(ref, ref, sem, qtr_sem.at[0], cross).wait_send()

    row64 = iota((SUB, PIECE), 0)
    lane64 = iota((SUB, PIECE), 1) % HEAD
    eye = row64 == lane64
    causal = row64 >= lane64
    low_head = iota((SUB, 128), 1) < HEAD

    def to_row(col):
        return jnp.sum(jnp.where(eye, col, 0.0), axis=0, keepdims=True)

    def to_col(row):
        return jnp.sum(jnp.where(eye[:, :HEAD], row[:, :HEAD], 0.0), axis=1, keepdims=True)

    def scale_of(square_sum):
        return lax.rsqrt(square_sum / inner + EPSILON) * (1.0 / 64.0)

    def inverse_of(square_sum):
        return jnp.where(square_sum < jnp.inf, 64.0 * jnp.sqrt(square_sum / inner + EPSILON), 0.0)

    def head_blocks(part):
        left, right = part[:, :128], part[:, 128:]
        none = jnp.zeros_like(left)
        rows = [jnp.concatenate([jnp.where(low_head, left, 0.0), none], axis=1), jnp.concatenate([jnp.where(low_head, 0.0, left), none], axis=1),
                jnp.concatenate([none, jnp.where(low_head, right, 0.0)], axis=1), jnp.concatenate([none, jnp.where(low_head, 0.0, right)], axis=1)]
        return jnp.concatenate(rows, axis=0).astype(BF16)

    def row_of(ref, layer, lanes=slice(None)):
        row = ref[0:1, lanes]
        for at in range(1, layers):
            row = jnp.where(layer == at, ref[at : at + 1, lanes], row)
        return row.astype(F32)

    def turn_wdt(layer):
        for k in range(0, wdt.shape[2], 128):
            block = wdt[layer, :, k : k + 128].astype(F32)
            turned = jnp.transpose(jnp.concatenate([block] * 3, axis=0)).astype(BF16)
            wbd[layer, k : k + 128, 2 * HEAD : 2 * HEAD + turned.shape[1]] = turned

    def start_layer():
        state[...] = jnp.zeros_like(state)
        x0s[0:8] = jnp.zeros((8, local), F32)
        q0s[0:8] = jnp.zeros((8, q0s.shape[1]), F32)

    def tap_sum(buf, size, lanes, kern, bias):
        total = bias
        for j in range(4):
            total = total + buf[5 + j : 5 + j + size, lanes] * kern[j : j + 1].astype(F32)
        return total

    def norm(layer, q, subs):
        square = [jnp.zeros((SUB, 1), F32) for _ in range(subs)]
        for r in range(subs):
            for side in range(2):
                for m in range(n_piece):
                    val = ubuf[layer, side, q + r, m]
                    square[r] = square[r] + jnp.sum(val * val, axis=1, keepdims=True)
        norm_row = row_of(nw, layer)
        for r in range(subs):
            scale = lax.rsqrt(square[r] / (2 * half) + EPSILON)
            for side in range(2):
                for m in range(n_piece):
                    at = side * half + m * PIECE
                    hbuf[r * SUB : (r + 1) * SUB, at : at + PIECE] = (ubuf[layer, side, q + r, m] * scale * norm_row[:, at : at + PIECE]).astype(BF16)

    def x_product(layer, size, n):
        x0s[8 : 8 + size, n * PIECE : (n + 1) * PIECE] = dot(hbuf[:size], wx[layer, n]).astype(BF16).astype(F32)

    def z_product(layer, size, n):
        zs[:size, n * PIECE : (n + 1) * PIECE] = jax.nn.silu(dot(hbuf[:size], wz[layer, n]).astype(BF16).astype(F32))

    def head(layer, q, subs, first, hook):
        size = subs * SUB
        if first:
            first_wait[0].wait()
        both = dot(hbuf[:size], wbd[layer]).astype(BF16).astype(F32)
        q0s[8 : 8 + size, :] = both[:, : 2 * HEAD]
        r_pre = both[:, 2 * HEAD : 2 * HEAD + 3 * (local // HEAD)]
        if first:
            for cp in smalls[1:-1]:
                cp.wait()
        if first:
            first_wait[1].wait()
        x_product(layer, size, 0)
        x_product(layer, size, 1)
        if not first:
            hook()
            x_product(layer, size, 2)
            x_product(layer, size, 3)
        bc = jax.nn.silu(tap_sum(q0s, size, slice(None), cbc[layer], row_of(bbc, layer)))
        q0s[0:8] = q0s[size : size + 8]
        triple = lambda ref: jnp.concatenate([row_of(ref, layer)] * 3, axis=1)
        dt_in = r_pre + triple(dtb)
        dt_val = jnp.maximum(dt_in, 0.0) + jnp.log1p(jnp.exp(-jnp.abs(dt_in)))
        a_vals = -dt_val * jnp.exp(triple(al))
        to_t, from_t = iota((size, 3 * size), 0), iota((size, 3 * size), 1) % size
        tri = jnp.where((to_t >= from_t) & (to_t // SUB == from_t // SUB), 1.0, 0.0).astype(BF16)
        a_cum = dot(tri, stack3(a_vals))
        skip = jnp.broadcast_to(triple(ds), (8, a_cum.shape[1]))
        to_spread = jnp.concatenate([dt_val, a_cum, skip], axis=0)
        hi, mid, lo = split3(to_spread)
        lane = iota(to_spread.shape, 1)
        n_heads = local // HEAD
        spread_in = jnp.where(lane < n_heads, hi, jnp.where(lane < 2 * n_heads, mid, lo)).astype(BF16)
        for n in range(n_piece):
            at = slice(n * PIECE, (n + 1) * PIECE)
            group = n * (PIECE // HEAD)
            pick = jnp.where(iota((3 * n_heads, PIECE), 1) // HEAD + group == iota((3 * n_heads, PIECE), 0) % n_heads, 1.0, 0.0).astype(BF16)
            spread[: 2 * size + 8, at] = dot(spread_in, pick)
        swapped = pltpu.roll(bc, HEAD, 1)
        turned = jnp.transpose(bc)
        c_stack, bt_stack, cb = [], [], []
        for r in range(subs):
            rows = slice(r * SUB, (r + 1) * SUB)
            c_stack.append(stack3(swapped[rows, :HEAD]))
            bt_stack.append(stack3(turned[:HEAD, rows]))
            cb.append(exact_dot(c_stack[r], [jnp.concatenate([part] * 4, axis=0).astype(BF16) for part in split3(bc[rows, :HEAD])], dot_nt))
        for r in range(subs):
            rows = slice(3 * r * SUB, 3 * (r + 1) * SUB)
            for n in range(n_piece):
                at = slice(n * PIECE, (n + 1) * PIECE)
                a_e = spread[size + r * SUB : size + (r + 1) * SUB, at]
                dstack[rows, at] = stack3(jnp.where(causal, jnp.exp(jnp.minimum(a_e - to_row(a_e), 0.0)), 0.0) * cb[r])

        def conv(n):
            at = slice(n * PIECE, (n + 1) * PIECE)
            xs[:size, at] = jax.nn.silu(tap_sum(x0s, size, at, cx[layer, :, at], row_of(bx, layer, at)))
            x0s[0:8, at] = x0s[size : size + 8, at]

        def inside(n):
            at = slice(n * PIECE, (n + 1) * PIECE)
            for r in range(subs):
                rows = slice(r * SUB, (r + 1) * SUB)
                x_dt = xs[rows, at] * spread[rows, at]
                ys[rows, at] = exact_dot(dstack[3 * r * SUB : 3 * (r + 1) * SUB, at], [head_blocks(part) for part in split3(x_dt)])

        def across(n):
            at = slice(n * PIECE, (n + 1) * PIECE)
            for r in range(subs):
                rows = slice(r * SUB, (r + 1) * SUB)
                a_e = spread[size + r * SUB : size + (r + 1) * SUB, at]
                a_last = a_e[SUB - 1 : SUB]
                old = state[:, at]
                carried = exact_dot(c_stack[r], [part.astype(BF16) for part in split3(old)])
                x_act = xs[rows, at]
                ys[rows, at] = ys[rows, at] + carried * jnp.exp(a_e) + spread[2 * size : 2 * size + 1, at] * x_act
                tail_x = x_act * spread[rows, at] * jnp.exp(a_last - a_e)
                state[:, at] = jnp.exp(a_last) * old + exact_dot(bt_stack[r], [part.astype(BF16) for part in split3(tail_x)])

        if first:
            conv(0)
            conv(1)
            first_wait[2].wait()
        plan = ORDER_FIRST if first else ORDER_LATER
        stages = {"x": lambda n: x_product(layer, size, n), "c": conv, "i": inside, "a": across, "z": lambda n: z_product(layer, size, n)}
        for step in plan:
            if step == "wait":
                first_wait[3].wait()
            else:
                stages[step[0]](int(step[1]))

    def tail(layer, q, subs, first):
        size = subs * SUB
        s = layer * n_subs + q
        gate_sq = jnp.zeros((size, 1), F32)
        for n in range(n_piece):
            at = slice(n * PIECE, (n + 1) * PIECE)
            v = ys[:size, at] * zs[:size, at]
            ys[:size, at] = v
            gate_sq = gate_sq + jnp.sum(v * v, axis=1, keepdims=True)
        scale = scale_of(gate_sq)
        gbuf[:size] = (ys[:size] * scale * row_of(gw, layer)).astype(BF16)
        for r in range(subs):
            pstat[core, s + r] = to_row(gate_sq[r * SUB : (r + 1) * SUB])[:, :128]
        if first:
            first_wait[4].wait()
        groups = [range(n_piece // 2), range(n_piece // 2, n_piece)] if first else [range(n_piece)]
        for pieces in groups:
            for m in pieces:
                part = dot(gbuf[:size], wo[layer, 1 - core, m])
                for r in range(subs):
                    psend[s + r, m] = part[r * SUB : (r + 1) * SUB]
            if first and pieces[0] == 0:
                pl.semaphore_wait(barrier, 2)
            for r in range(subs):
                if pieces[0] == 0:
                    pstat_copy(s + r).start()
                for m in pieces:
                    p_copy(s + r, m).start()
        if first:
            first_wait[5].wait()
        for m in range(n_piece):
            part = dot(gbuf[:size], wo[layer, core, m])
            for r in range(subs):
                own[m] = part[r * SUB : (r + 1) * SUB]

    def combine(s):
        pstat_copy(s).wait_recv()
        own_sq = to_col(pstat[core, s])
        peer_sq = to_col(pstat[1 - core, s])
        chip_sq = own_sq + peer_sq
        chip_scale = scale_of(chip_sq)
        f_own = chip_scale * inverse_of(own_sq)
        f_peer = chip_scale * inverse_of(peer_sq)
        qstat[chip, s] = to_row(chip_sq)[:, :128]
        qstat_copy(s).start()
        for m in range(n_piece):
            if m % 2 == 0:
                pair = pl.ds(m, 2)
                remote(psend.at[s, pair], prcv.at[s, pair], 0, pr_sem.at[s % 2, m // 2], peer).wait_recv()
            qbuf[chip, s, m] = own[m] * f_own + prcv[s, m] * f_peer
            q_copy(s, m).start()

    def update(s, pieces=False):
        layer, c = s // n_subs, s % n_subs
        qstat_copy(s).wait_recv()
        if not pieces:
            q_arrived(s)
        sq0 = to_col(qstat[0, s])
        sq1 = to_col(qstat[1, s])
        norm = lax.rsqrt((sq0 + sq1) / inner + EPSILON)
        f0 = norm * inverse_of(sq0)
        f1 = norm * inverse_of(sq1)
        for m in range(n_piece):
            if pieces:
                q_copy(s, m).wait_recv()
            total = ubuf[layer, core, c, m] + (qbuf[0, s, m] * f0 + qbuf[1, s, m] * f1)
            ubuf[layer + 1, core, c, m] = total.astype(BF16).astype(F32)
            u_copy(s, m).start()

    def emit(s, pieces=False):
        c = s % n_subs
        for side in (core, 1 - core):
            if side is not core and not pieces:
                u_arrived(s)
            for m in range(n_piece):
                if side is not core and pieces:
                    u_copy(s, m).wait_recv()
                cols = pl.ds(pl.multiple_of(side * half + m * PIECE, PIECE), PIECE)
                out_ref[0, pl.ds(pl.multiple_of(c * SUB, SUB), SUB), cols] = ubuf[layers, side, c, m].astype(BF16)

    def load_hidden(c):
        hid_copy(c).wait()
        for side in range(2):
            for m in range(n_piece):
                at = side * half + m * PIECE
                ubuf[0, side, c, m] = hid[c, :, at : at + PIECE].astype(F32)

    steps = layers * n_subs
    lag = n_subs - 1
    steps = layers * n_subs
    lag = n_subs - 1
    start_layer()
    smalls[0].wait()
    smalls[-1].wait()
    turn_wdt(0)
    load_hidden(0)
    norm(0, 0, 1)
    head(0, 0, 1, True, lambda: None)
    tail(0, 0, 1, True)

    bc_copy(1).start()
    start_weights(1)
    combine(0)

    @pl.loop(1, steps)
    def _(t):
        layer, q = t // n_subs, t % n_subs

        @pl.when(t < n_subs)
        def _():
            load_hidden(q)

        @pl.when(t >= n_subs)
        def _():
            u_arrived(t - n_subs)

        for at in range(1, layers):
            @pl.when(t == at * n_subs)
            def _():
                start_layer()
                turn_wdt(at)
                for cp in weight_waits(at):
                    cp.wait()
                if at + 1 < layers:
                    bc_copy(at + 1).start()
                    start_weights(at + 1)

        norm(layer, q, 1)

        @pl.when(t == 2)
        def _():
            combine(t - 1)

        @pl.when(t >= lag)
        def _():
            update(t - lag)

        def hook():
            @pl.when(t > 2)
            def _():
                combine(t - 1)

        head(layer, q, 1, False, hook)
        tail(layer, q, 1, False)

    combine(steps - 1)
    final = steps - n_subs

    @pl.loop(final, steps - 1)
    def _(s):
        @pl.when(s > final)
        def _():
            emit(s - 1)

        @pl.when(s > steps - 1 - lag)
        def _():
            update(s)

    emit(steps - 2)
    update(steps - 1, True)
    emit(steps - 1, True)
    all_sent()


def solution(mesh):
    in_specs = (P('dp'), P(), P(None, None, 'tp'), P(None, None, 'tp'), P(), P(None, None, 'tp'), P(None, None, 'tp'), P(), P(None, 'tp'), P(),
                P(None, 'tp'), P(None, 'tp'), P(None, 'tp'), P(None, 'tp'), P(None, 'tp', None))
    tp_size = mesh.shape['tp']

    def device_forward(hidden, norm_w, w_z, w_x, w_bc, w_dt, conv_x, conv_bc, bias_x, bias_bc, dt_bias, a_log, d_skip, gate_w, w_out):
        layers, width, local = w_x.shape
        n_subs = hidden.shape[1] // SUB
        n_piece = local // PIECE
        steps = layers * n_subs
        bc_width = w_bc.shape[-1]
        w_dt = jnp.swapaxes(w_dt, 1, 2)
        vm = lambda shape, dtype: pltpu.VMEM(shape, dtype)
        same = lambda arr: pltpu.VMEM(arr.shape, arr.dtype)
        scratch = [
            vm((n_subs, SUB, width), BF16), same(norm_w), vm((layers, n_piece, width, PIECE), BF16), vm((layers, n_piece, width, PIECE), BF16),
            vm((layers, width, PIECE), BF16), same(w_dt), same(conv_x), same(conv_bc), same(bias_x), same(bias_bc), same(dt_bias), same(a_log), same(d_skip), same(gate_w),
            vm((layers, 2, n_piece, local, PIECE), BF16),
            vm((layers + 1, 2, n_subs, n_piece, SUB, PIECE), F32),
            vm((steps, n_piece, SUB, PIECE), F32), vm((steps, n_piece, SUB, PIECE), F32), vm((2, steps, n_piece, SUB, PIECE), F32),
            vm((2, steps, 1, 128), F32), vm((2, steps, 1, 128), F32),
            vm((n_piece, SUB, PIECE), F32), vm((MAX_ROWS, width), BF16), vm((MAX_ROWS + 8, local), F32), vm((MAX_ROWS + 8, bc_width), F32),
            vm((MAX_ROWS, local), F32), vm((MAX_ROWS, local), F32), vm((MAX_ROWS, local), F32), vm((3 * MAX_ROWS, local), BF16), vm((2 * MAX_ROWS + 8, local), F32), vm((HEAD, local), F32), vm((MAX_ROWS, local), BF16),
            pltpu.SemaphoreType.DMA((10,)), pltpu.SemaphoreType.DMA((n_subs,)), pltpu.SemaphoreType.DMA((6,)), pltpu.SemaphoreType.DMA((5,)),
            pltpu.SemaphoreType.DMA((2, n_piece // 2)), pltpu.SemaphoreType.DMA((steps - 1 + n_piece,)), pltpu.SemaphoreType.DMA((steps - 1 + n_piece,)),
            pltpu.SemaphoreType.DMA((2,)), pltpu.SemaphoreType.DMA((steps,)),
        ]
        return pl.pallas_call(
            functools.partial(kernel, float(local * tp_size)),
            out_shape=jax.ShapeDtypeStruct(hidden.shape, hidden.dtype),
            in_specs=[pl.BlockSpec(memory_space=pltpu.HBM)] * 15,
            out_specs=pl.BlockSpec(memory_space=pltpu.VMEM),
            scratch_shapes=scratch,
            compiler_params=pltpu.CompilerParams(collective_id=0, has_side_effects=True, vmem_limit_bytes=52 * 1024 * 1024),
        )(*[pltpu.with_memory_space_constraint(arr, pltpu.HBM) for arr in (hidden, norm_w, w_z, w_x, w_bc, w_dt, conv_x, conv_bc, bias_x, bias_bc, dt_bias, a_log, d_skip, gate_w, w_out)])

    return jax.shard_map(device_forward, mesh=mesh, in_specs=in_specs, out_specs=P('dp'), check_vma=False)
```
